256 devices in a mesh: ctg: 32 (over x, y, core), br: 8 (over z).
Axes of the slice: x: 4, y: 4, z: 8, core: 2. Of those that a mesh axis runs over, the one named last changes fastest.
Arguments:
- base_vm: float32 [10240], P(('ctg', 'br')), may hold values from 0.95 to 1.05
- base_va: float32 [10240], P(('ctg', 'br')), may hold values from -0.6 to 0.6
- delta_state: float32 [256, 2, 10240], P('ctg', None, 'br'), may hold values from -0.18 to 0.18
- multipliers: float32 [256, 2, 10240], P('ctg', None, 'br'), may hold values from -6 to 6
- net_inj: float32 [256, 2, 10240], P('ctg', None, 'br'), may hold values from -6 to 6
- ang_grad: float32 [256, 10240], P('ctg', 'br'), may hold values from -6 to 6
- from_bus: int32 [13312], P('br'), may hold values from 0 to 10239
- to_bus: int32 [13312], P('br'), may hold values from 0 to 10239
- status: int32 [256, 13312], P('ctg', 'br'), may hold values 0 or 1
- conduct: float32 [13312], P('br'), may hold values from 1 to 5
- suscept: float32 [13312], P('br'), may hold values from -15 to -5
- charging: float32 [13312], P('br'), may hold values from 0.1 to 0.6
- rating: float32 [13312], P('br'), may hold values from 1 to 3
- slack: float32 [256, 13312], P('ctg', 'br'), may hold values from 0.05 to 2
- zdual: float32 [256, 13312], P('ctg', 'br'), may hold values from 0.05 to 2
Outputs:
- mismatch: float32 [256, 2, 10240], P('ctg', None, 'br')
- dual_res: float32 [256, 10240], P('ctg', 'br')
- limit_res: float32 [256, 13312], P('ctg', 'br')
- ctg_norms: float32 [256, 4], P('ctg')
- total_norms: float32 [4], replicated
The draws below stay inside these ranges and needn't reach their ends.
All inputs are finite; a program needn't handle non-finite values. No bound on the sum of `status` on one device may be relied on, other than what follows from the above.
Results may differ from the reference program's by a relative error of at most 0.0003.
Values sent between devices are 32-bit elements; how exact they have to be, the bound alone decides.
A program may use at most 64 MiB of HBM per device.

```python
import math
import jax
import jax.numpy as jnp
from jax import lax

NB = 10240
NL = 13312
CTG = 256


def place_ends(drawn, rng, smallest, high):
    longest = drawn.shape.index(max(drawn.shape))
    spots = []
    for shift in (0, 1):
        where = [jax.random.randint(jax.random.fold_in(rng, axis), (), 0, length) for axis, length in enumerate(drawn.shape)]
        where[longest] = (where[longest] + shift) % drawn.shape[longest]
        spots.append(tuple(where))
    return drawn.at[spots[0]].set(smallest).at[spots[1]].set(high)


def shard_levels(key, extent, shards, low, top_value):
    def one(position, shards_of):
        draws = jax.random.uniform(jax.random.fold_in(jax.random.fold_in(key, 6), position), (shards_of,), jnp.float32, low / len(shards), top_value / len(shards))
        return jnp.repeat(jnp.exp(draws), extent[position] // shards_of).reshape((-1,) + (1,) * (len(extent) - position - 1))

    loudness = one(*shards[0])
    for cut in shards[1:]:
        loudness = loudness * one(*cut)
    return loudness


def gaussian(key, extent, width, limit, split=(), dtype=jnp.bfloat16):
    array = jax.random.normal(key, extent, jnp.float32) * width
    if len(split) > 0:
        array = shard_levels(key, extent, split, -0.22, 0.18) * array
    return jnp.clip(array, min=-limit, max=limit).astype(dtype)


def setup_inputs(seed: int = 0) -> dict:
    streams_of = jax.random.split(jax.random.key(seed), 16)
    base_vm = jnp.clip(0.95 + 0.099999964 * jax.random.uniform(streams_of[0], (NB,), jnp.float32) ** shard_levels(streams_of[0], (NB,), ((0, 256),), -0.2, 0.2), 0.95, 1.05)
    base_va = gaussian(streams_of[1], (NB,), 0.1, 0.6, ((0, 256),), jnp.float32)
    delta_state = gaussian(streams_of[2], (CTG, 2, NB), 0.03, 0.18, ((0, 32), (2, 8)), jnp.float32)
    multipliers = gaussian(streams_of[3], (CTG, 2, NB), 1.0, 6.0, ((0, 32), (2, 8)), jnp.float32)
    net_inj = gaussian(streams_of[4], (CTG, 2, NB), 1.0, 6.0, ((0, 32), (2, 8)), jnp.float32)
    ang_grad = gaussian(streams_of[5], (CTG, NB), 1.0, 6.0, ((0, 32), (1, 8)), jnp.float32)
    from_bus = place_ends(jax.random.randint(streams_of[6], (NL,), 0, NB), jax.random.fold_in(streams_of[6], 1), 0, NB - 1).astype(jnp.int32)
    to_bus = place_ends(jax.random.randint(streams_of[7], (NL,), 0, NB), jax.random.fold_in(streams_of[7], 1), 0, NB - 1).astype(jnp.int32)
    status = place_ends((jax.random.randint(streams_of[8], (CTG, NL), 0, 8) < 7).astype(jnp.int32), jax.random.fold_in(streams_of[8], 1), 0, 1)
    conduct = jnp.clip(1.0 + 4.0 * jax.random.uniform(streams_of[9], (NL,), jnp.float32) ** shard_levels(streams_of[9], (NL,), ((0, 8),), -0.2, 0.2), 1.0, 5.0)
    suscept = jnp.clip(-15.0 + 10.0 * jax.random.uniform(streams_of[10], (NL,), jnp.float32) ** shard_levels(streams_of[10], (NL,), ((0, 8),), -0.2, 0.2), -15.0, -5.0)
    charging = jnp.clip(0.1 + 0.5 * jax.random.uniform(streams_of[11], (NL,), jnp.float32) ** shard_levels(streams_of[11], (NL,), ((0, 8),), -0.2, 0.2), 0.1, 0.6)
    rating = jnp.clip(1.0 + 2.0 * jax.random.uniform(streams_of[12], (NL,), jnp.float32) ** shard_levels(streams_of[12], (NL,), ((0, 8),), -0.2, 0.2), 1.0, 3.0)
    slack = jnp.clip(jnp.exp(math.log(2.0) - 3.6888794 * jax.random.uniform(streams_of[13], (CTG, NL), jnp.float32) ** shard_levels(streams_of[13], (CTG, NL), ((0, 32), (1, 8)), -0.2, 0.2)), 0.05, 2.0)
    zdual = jnp.clip(jnp.exp(math.log(2.0) - 3.6888794 * jax.random.uniform(streams_of[14], (CTG, NL), jnp.float32) ** shard_levels(streams_of[14], (CTG, NL), ((0, 32), (1, 8)), -0.2, 0.2)), 0.05, 2.0)
    return dict(base_vm=base_vm, base_va=base_va, delta_state=delta_state, multipliers=multipliers, net_inj=net_inj, ang_grad=ang_grad, from_bus=from_bus, to_bus=to_bus, status=status, conduct=conduct, suscept=suscept, charging=charging, rating=rating, slack=slack, zdual=zdual)


def branch_flows(volt_mag, volt_ang, mult_p, mult_q, from_idx, to_idx, conduct, suscept, charging, in_service):
    volt_from = volt_mag[:, from_idx]
    volt_to = volt_mag[:, to_idx]
    angle_diff = volt_ang[:, from_idx] - volt_ang[:, to_idx]
    cos_diff = jnp.cos(angle_diff)
    sin_diff = jnp.sin(angle_diff)
    volt_prod = volt_from * volt_to
    p_from = conduct * volt_from * volt_from - volt_prod * (conduct * cos_diff + suscept * sin_diff)
    q_from = -(suscept + charging) * volt_from * volt_from - volt_prod * (conduct * sin_diff - suscept * cos_diff)
    p_to = conduct * volt_to * volt_to - volt_prod * (conduct * cos_diff - suscept * sin_diff)
    q_to = -(suscept + charging) * volt_to * volt_to + volt_prod * (conduct * sin_diff + suscept * cos_diff)
    flow_dual = volt_prod * (mult_p[:, from_idx] * (conduct * sin_diff - suscept * cos_diff) - mult_q[:, from_idx] * (conduct * cos_diff + suscept * sin_diff) + mult_p[:, to_idx] * (conduct * sin_diff + suscept * cos_diff) + mult_q[:, to_idx] * (conduct * cos_diff - suscept * sin_diff))
    at_from = jnp.stack([p_from, q_from, flow_dual], 1) * in_service[:, None, :]
    at_to = jnp.stack([p_to, q_to, -flow_dual], 1) * in_service[:, None, :]
    return (at_from, at_to)

def reference(base_vm, base_va, delta_state, multipliers, net_inj, ang_grad, from_bus, to_bus, status, conduct, suscept, charging, rating, slack, zdual):
    volt_mag = base_vm[None, :] + delta_state[:, 0]
    volt_ang = base_va[None, :] + delta_state[:, 1]
    in_service = status.astype(jnp.float32)
    at_from, at_to = branch_flows(volt_mag, volt_ang, multipliers[:, 0], multipliers[:, 1], from_bus, to_bus, conduct, suscept, charging, in_service)
    scenarios = delta_state.shape[0]
    buses = delta_state.shape[2]
    summed = jnp.zeros((scenarios, 3, buses), jnp.float32)
    summed = summed.at[:, :, from_bus].add(at_from).at[:, :, to_bus].add(at_to)
    mismatch = summed[:, :2] - net_inj
    dual_res = summed[:, 2] + ang_grad
    limit_res = in_service * (at_from[:, 0] * at_from[:, 0] + at_from[:, 1] * at_from[:, 1] + slack - rating * rating)
    complement = in_service * (zdual * slack - 0.01)
    squares = jnp.stack([lax.optimization_barrier(jnp.sum(mismatch * mismatch, axis=(1, 2))), lax.optimization_barrier(jnp.sum(dual_res * dual_res, axis=1)), lax.optimization_barrier(jnp.sum(limit_res * limit_res, axis=1)), lax.optimization_barrier(jnp.sum(complement * complement, axis=1))], 1)
    ctg_norms = jnp.sqrt(squares)
    total_norms = jnp.sqrt(lax.optimization_barrier(jnp.sum(squares, axis=0)) / scenarios)
    return (mismatch, dual_res, limit_res, ctg_norms, total_norms)
```

```python
import functools

import jax
import jax.numpy as jnp
from jax import lax
from jax.experimental import pallas as pl
from jax.experimental.pallas import tpu as pltpu
from jax.sharding import PartitionSpec as P

LANES = 128
SUB = 8
SPAN = 256
MESH = pl.DeviceIdType.MESH

ENDS, PARAMS, STATUS, MULT, DELTA, PIECE, BASE, NET, WORK, ANG, COMP, ENDS2, PARAMS2, SQ, MIS, DUAL, LIM, TOTAL = range(18)
KINDS = 18


def sin_cos(x):
    y = x * x
    sin_c = (1 / 6227020800, -1 / 39916800, 1 / 362880, -1 / 5040, 1 / 120, -1 / 6)
    cos_c = (-1 / 87178291200, 1 / 479001600, -1 / 3628800, 1 / 40320, -1 / 720, 1 / 24, -0.5)
    s = jnp.full_like(y, sin_c[0])
    for c in sin_c[1:]:
        s = s * y + c
    k = jnp.full_like(y, cos_c[0])
    for c in cos_c[1:]:
        k = k * y + c
    return x + x * y * s, 1.0 + y * k


def body(
    groups, ranks,
    vm_any, va_any, delta_any, mult_any, net_any, ang_any, from_any, to_any,
    g_any, b_any, h_any, rating_any, status_any, slack_any, zdual_any,
    mis_out, dual_out, lim_out, norm_out, tot_out,
    vm1, va1, dstg, mstg, nstg, ang8, st8, sl8, zd8, rate,
    ststg, wstg, astg, cstg,
    ebuf, pbuf, stbuf, mbuf, dbuf, zbuf, cbuf, nbuf, wbuf, abuf, compbuf,
    table, dends, dpar, dst, dwork, dlim, acc,
    mout, dout, lout, min_, din, lin, sqbuf, rowbuf,
    local, send, recv,
):
    grp, me = lax.axis_index("ctg"), lax.axis_index("br")
    core = lax.rem(grp, 2)
    sibling = grp + 1 - 2 * core
    scen, _, nb = delta_any.shape
    rows = from_any.shape[0]
    btiles = nb // LANES
    tiles = table.shape[1]
    f32, bf16 = jnp.float32, jnp.bfloat16
    piece_len = vm_any.shape[1]

    def fetch(i, src, dst):
        copy = pltpu.make_async_copy(src, dst, local.at[i])
        copy.start()
        return copy

    ends_in = [pltpu.make_async_copy(src, ebuf.at[me, i], local.at[2 + i]) for i, src in enumerate((from_any, to_any))]
    params_in = [pltpu.make_async_copy(src, pbuf.at[me, i], local.at[8 + i]) for i, src in enumerate((g_any, b_any, h_any))]

    @pl.when(core == 0)
    def _():
        for copy in ends_in:
            copy.start()

    @pl.when(core == 1)
    def _():
        for copy in params_in:
            copy.start()

    base_in = [fetch(0, vm_any, vm1), fetch(1, va_any, va1)]
    status_in = [fetch(4, status_any, st8), fetch(5, slack_any, sl8), fetch(6, zdual_any, zd8), fetch(7, rating_any, rate)]
    bus_in = [fetch(11, delta_any, dstg), fetch(12, mult_any, mstg)]
    late_in = [fetch(13, net_any, nstg), fetch(14, ang_any, ang8)]

    barrier = pltpu.get_barrier_semaphore()

    def greet_near(i, carry):
        pl.semaphore_signal(barrier, inc=1, device_id=(grp, lax.rem(me + i, ranks)), device_id_type=MESH)
        return carry

    def greet_far(i, carry):
        pl.semaphore_signal(barrier, inc=1, device_id=(lax.rem(grp + i, groups), me), device_id_type=MESH)
        return carry

    lax.fori_loop(1, ranks, greet_near, 0)
    lax.fori_loop(1, groups, greet_far, 0)

    for copy in base_in + status_in:
        copy.wait()

    lane = lax.broadcasted_iota(jnp.int32, (SUB, LANES), 1)
    pad = jnp.zeros((1, LANES - piece_len), f32)
    piece = jnp.concatenate(
        [jnp.concatenate([vm1[...], pad], axis=1), jnp.concatenate([va1[...], pad], axis=1), jnp.zeros((SUB - 2, LANES), f32)],
        axis=0,
    )
    shift = lax.rem(grp * (ranks * piece_len) + me * piece_len, LANES)
    piece = pltpu.roll(piece, shift, 1)
    zbuf[me] = piece[0:2, :]

    for r in range(rows):
        cols = slice(r * LANES, (r + 1) * LANES)
        ststg[:, r, :] = st8[:, cols]
        wstg[:, r, :] = sl8[:, cols]
    squared = rate[...] * rate[...]
    for s in range(scen):
        wstg[s] = wstg[s] - squared
    comp = st8[...].astype(f32) * (zd8[...] * sl8[...] - 0.01)
    cstg[:, 0, :] = jnp.broadcast_to(jnp.sum(comp * comp, axis=1, keepdims=True), (scen, LANES))

    for copy in bus_in + late_in:
        copy.wait()
    for k in range(btiles):
        astg[:, k, :] = ang8[:, k * LANES : (k + 1) * LANES]

    pl.semaphore_wait(barrier, ranks - 1 + groups - 1)

    def near(kind, step, src, dst):
        pltpu.make_async_remote_copy(
            src_ref=src, dst_ref=dst, send_sem=send.at[kind], recv_sem=recv.at[kind],
            device_id=(grp, lax.rem(me + step, ranks)), device_id_type=MESH,
        ).start()

    def far(kind, step, src, dst):
        pltpu.make_async_remote_copy(
            src_ref=src, dst_ref=dst, send_sem=send.at[kind], recv_sem=recv.at[kind],
            device_id=(lax.rem(grp + step, groups), me), device_id_type=MESH,
        ).start()

    def across(kind, ref):
        return pltpu.make_async_remote_copy(
            src_ref=ref, dst_ref=ref, send_sem=send.at[kind], recv_sem=recv.at[kind],
            device_id=(sibling, me), device_id_type=MESH,
        )

    def whole(kind, ref, n):
        part = ref.at[pl.ds(0, n)]
        return pltpu.make_async_remote_copy(
            src_ref=part, dst_ref=part, send_sem=send.at[kind], recv_sem=recv.at[kind],
            device_id=(sibling, me), device_id_type=MESH,
        )

    def to_near(kind, src_of, dst):
        def go(step, carry):
            near(kind, step, src_of(lax.rem(me + step, ranks)), dst)
            return carry
        lax.fori_loop(1, ranks, go, 0)

    def to_far(kind, src, dst):
        def go(step, carry):
            far(kind, step, src, dst)
            return carry
        lax.fori_loop(1, groups, go, 0)

    to_near(PIECE, lambda p: zbuf.at[me], zbuf.at[me])

    @pl.when(core == 0)
    def _():
        for copy in ends_in:
            copy.wait()
        to_near(ENDS, lambda p: ebuf.at[me], ebuf.at[me])

    @pl.when(core == 1)
    def _():
        for copy in params_in:
            copy.wait()
        to_near(PARAMS, lambda p: pbuf.at[me], pbuf.at[me])

    to_near(STATUS, lambda p: ststg.at[p], stbuf.at[me])
    to_near(DELTA, lambda p: dstg.at[p], dbuf.at[me])
    to_near(MULT, lambda p: mstg.at[p], mbuf.at[me])
    to_near(COMP, lambda p: cstg.at[p], compbuf.at[me])
    to_near(NET, lambda p: nstg.at[p], nbuf.at[me])
    to_near(WORK, lambda p: wstg.at[p], wbuf.at[me])
    to_near(ANG, lambda p: astg.at[p], abuf.at[me])

    stbuf[me] = ststg[me]
    dbuf[me] = dstg[me]
    mbuf[me] = mstg[me]
    nbuf[me] = nstg[me]
    wbuf[me] = wstg[me]
    abuf[me] = astg[me]
    compbuf[me] = cstg[me]
    acc[...] = jnp.zeros_like(acc)

    whole(PIECE, zbuf, ranks - 1).wait_recv()
    window = (LANES // 2) * core
    for m in range(3):
        off = m * LANES + lane[0:2, :] - window
        found = jnp.zeros((2, LANES), f32)
        for b in range(ranks):
            inside = (off >= b * piece_len) & (off < (b + 1) * piece_len)
            found = jnp.where(inside, zbuf[b], found)
        cbuf[grp, m : m + 1, :] = found[0:1, :]
        cbuf[grp, 3 + m : 4 + m, :] = found[1:2, :]
    cbuf[grp, 6:8, :] = jnp.zeros((2, LANES), f32)
    to_far(BASE, cbuf.at[grp], cbuf.at[grp])

    @pl.when(core == 0)
    def _():
        whole(ENDS, ebuf, ranks - 1).wait_recv()
        across(ENDS2, ebuf).start()

    @pl.when(core == 1)
    def _():
        whole(PARAMS, pbuf, ranks - 1).wait_recv()
        across(PARAMS2, pbuf).start()
        across(ENDS2, ebuf).wait_recv()

    for end in range(2):
        for z in range(ranks):
            dends[end, z * rows : (z + 1) * rows, :] = ebuf[z, end]

    whole(MULT, mbuf, ranks - 1).wait_recv()
    for z in range(ranks):
        for q in range(2):
            for k in range(btiles):
                at = z * btiles + k
                table[2 + q, at : at + 1, :] = mbuf[z, q : q + 1, k * LANES : (k + 1) * LANES]

    whole(STATUS, stbuf, ranks - 1).wait_recv()
    for z in range(ranks):
        dst[z * rows : (z + 1) * rows, :] = stbuf[z]

    @pl.when(core == 0)
    def _():
        across(PARAMS2, pbuf).wait_recv()

    for q in range(3):
        for z in range(ranks):
            dpar[q, z * rows : (z + 1) * rows, :] = pbuf[z, q]

    whole(DELTA, dbuf, ranks - 1).wait_recv()
    whole(BASE, cbuf, groups - 1).wait_recv()
    for r in range(groups // 2):
        for q in range(2):
            def one(c, m):
                return cbuf[2 * r + c, 3 * q + m : 3 * q + m + 1, :]
            five = (one(0, 0), one(0, 1), one(0, 2) + one(1, 0), one(1, 1), one(1, 2))
            for m in range(5):
                at = 5 * r + m
                z, k = at // btiles, at % btiles
                table[q, at : at + 1, :] = five[m] + dbuf[z, q : q + 1, k * LANES : (k + 1) * LANES]

    chunks = dends.shape[1] // SUB
    high = acc.shape[0] // 6
    used = tiles * LANES // SPAN
    label = lax.broadcasted_iota(jnp.int32, (SPAN, LANES), 0).astype(bf16)
    steps = lax.broadcasted_iota(jnp.int32, (high, LANES), 0).astype(bf16)

    def at_rows(i):
        return pl.ds(pl.multiple_of(i * SUB, SUB), SUB)

    def pick(i):
        picked = []
        for end in range(2):
            spot = dends[end, at_rows(i), :]
            low, tile = spot & (LANES - 1), spot >> 7
            found = [jnp.zeros((SUB, LANES), f32) for _ in range(4)]
            for k in range(tiles):
                here = tile == k
                for q in range(4):
                    row = jnp.broadcast_to(table[q, k : k + 1, :], (SUB, LANES))
                    got = jnp.take_along_axis(row, low, axis=1, mode="promise_in_bounds")
                    found[q] = jnp.where(here, got, found[q])
            picked += found
        return tuple(picked)

    def spread(x, n):
        return jnp.concatenate([jnp.broadcast_to(x, (2 * SUB, LANES)).astype(bf16)] * (n // (2 * SUB)), axis=0)

    def process(i, picked):
        vf, af, mpf, mqf, vt, at, mpt, mqt = picked
        where_ = at_rows(i)
        sn, cs = sin_cos(af - at)
        g, b, h = dpar[0, where_, :], dpar[1, where_, :], dpar[2, where_, :]
        live = dst[where_, :].astype(f32)
        u = vf * vt
        gc_bs, gc_mbs = g * cs + b * sn, g * cs - b * sn
        gs_bc, gs_mbc = g * sn + b * cs, g * sn - b * cs
        bh = -(b + h)
        pf = live * (g * vf * vf - u * gc_bs)
        qf = live * (bh * vf * vf - u * gs_mbc)
        pt = live * (g * vt * vt - u * gc_mbs)
        qt = live * (bh * vt * vt + u * gs_bc)
        fd = live * u * (mpf * gs_mbc - mqf * gc_bs + mpt * gs_bc + mqt * gc_mbs)
        dlim[where_, :] = pf * pf + qf * qf
        total = None
        for end, terms in ((0, (pf, qf, fd)), (1, (pt, qt, -fd))):
            parts = []
            for value in terms:
                head = value.astype(bf16).astype(f32)
                parts += [head, value - head]
            spot = dends[end, where_, :]
            low, tile = spot & (SPAN - 1), spot >> 8
            lefts, hots = [], []
            for r in range(SUB):
                row = slice(r, r + 1)
                mask = spread(tile[row, :], high) == steps
                lefts.append(jnp.concatenate(
                    [jnp.where(mask, spread(x[row, :], high), bf16(0)) for x in parts], axis=0
                ))
                hots.append(jnp.where(spread(low[row, :], SPAN) == label, bf16(1), bf16(0)))
            dot = lax.dot_general(
                jnp.concatenate(lefts, axis=1), jnp.concatenate(hots, axis=1),
                (((1,), (1,)), ((), ())), preferred_element_type=f32,
            )
            total = dot if total is None else total + dot
        acc[...] += total

    def advance(i, picked):
        following = pick(i + 1)
        process(i, picked)
        return following

    process(chunks - 1, lax.fori_loop(0, chunks - 1, advance, pick(0)))

    whole(NET, nbuf, ranks - 1).wait_recv()
    whole(WORK, wbuf, ranks - 1).wait_recv()
    whole(ANG, abuf, ranks - 1).wait_recv()
    whole(COMP, compbuf, ranks - 1).wait_recv()

    per = nb // SPAN
    mis_sq = jnp.zeros((1, SPAN), f32)
    dual_sq = jnp.zeros((1, LANES), f32)
    for z in range(ranks):
        for j in range(per):
            t = z * per + j
            cols = slice(j * SPAN, (j + 1) * SPAN)
            for q in range(3):
                top, bottom = (2 * q) * high + t, (2 * q + 1) * high + t
                row = acc[top : top + 1, :] + acc[bottom : bottom + 1, :]
                if q < 2:
                    row = row - nbuf[z, q : q + 1, cols]
                    mout[z, q : q + 1, cols] = row
                    mis_sq = mis_sq + row * row
                else:
                    for half in range(2):
                        k = 2 * j + half
                        one = row[:, half * LANES : (half + 1) * LANES] + abuf[z, k : k + 1, :]
                        dout[z, k : k + 1, :] = one
                        dual_sq = dual_sq + one * one
    lim_sq = jnp.zeros((rows, LANES), f32)
    for z in range(ranks):
        lim = stbuf[z].astype(f32) * (dlim[z * rows : (z + 1) * rows, :] + wbuf[z])
        lout[z] = lim
        lim_sq = lim_sq + lim * lim
    comp_sq = jnp.zeros((1, LANES), f32)
    for z in range(ranks):
        comp_sq = comp_sq + compbuf[z]

    def total_of(x):
        return jnp.sum(jnp.sum(x, axis=0, keepdims=True), axis=1, keepdims=True)

    lane1 = lane[0:1, :]
    squares = jnp.where(
        lane1 == 0, total_of(mis_sq),
        jnp.where(lane1 == 1, total_of(dual_sq), jnp.where(lane1 == 2, total_of(lim_sq), jnp.where(lane1 == 3, comp_sq, 0.0))),
    )
    sqbuf[me] = squares
    to_near(SQ, lambda p: sqbuf.at[me], sqbuf.at[me])
    to_near(MIS, lambda p: mout.at[p], min_.at[me])
    to_near(DUAL, lambda p: dout.at[p], din.at[me])
    to_near(LIM, lambda p: lout.at[p], lin.at[me])
    min_[me] = mout[me]
    din[me] = dout[me]
    lin[me] = lout[me]

    whole(SQ, sqbuf, ranks - 1).wait_recv()
    column = jnp.zeros((1, LANES), f32)
    for z in range(ranks):
        one = sqbuf[z]
        column = column + one
        norm_out[z : z + 1, :] = jnp.sqrt(one[:, 0:4])
    rowbuf[grp] = column
    to_far(TOTAL, rowbuf.at[grp], rowbuf.at[grp])

    whole(MIS, min_, ranks - 1).wait_recv()
    mis_out[...] = min_[...]
    whole(DUAL, din, ranks - 1).wait_recv()
    for k in range(btiles):
        dual_out[:, k * LANES : (k + 1) * LANES] = din[:, k, :]
    whole(LIM, lin, ranks - 1).wait_recv()
    for r in range(rows):
        lim_out[:, r * LANES : (r + 1) * LANES] = lin[:, r, :]

    @pl.when(core == 0)
    def _():
        whole(ENDS, ebuf, ranks - 1).wait_send()
        across(ENDS2, ebuf).wait_send()

    @pl.when(core == 1)
    def _():
        whole(PARAMS, pbuf, ranks - 1).wait_send()
        across(PARAMS2, pbuf).wait_send()

    for kind, ref in (
        (PIECE, zbuf), (STATUS, ststg), (DELTA, dstg), (MULT, mstg), (COMP, cstg), (NET, nstg), (WORK, wstg),
        (ANG, astg), (SQ, sqbuf), (MIS, mout), (DUAL, dout), (LIM, lout),
    ):
        whole(kind, ref, ranks - 1).wait_send()
    whole(BASE, cbuf, groups - 1).wait_send()
    whole(TOTAL, rowbuf, groups - 1).wait_send()

    whole(TOTAL, rowbuf, groups - 1).wait_recv()
    everything = jnp.zeros((1, LANES), f32)
    for i in range(groups):
        everything = everything + rowbuf[i]
    tot_out[...] = jnp.sqrt(everything[:, 0:4] / (scen * groups))


def per_device(
    base_vm, base_va, delta_state, multipliers, net_inj, ang_grad, from_bus, to_bus,
    status, conduct, suscept, charging, rating, slack, zdual,
):
    groups, ranks = lax.axis_size("ctg"), lax.axis_size("br")
    scen, _, nb = delta_state.shape
    nl = from_bus.shape[0]
    rows, btiles = nl // LANES, nb // LANES
    buses = nb * ranks
    tiles = buses // LANES
    high = -(-(buses // SPAN) // 16) * 16
    block = base_vm.shape[0]
    f32, i32 = jnp.float32, jnp.int32
    vmem = pl.BlockSpec(memory_space=pltpu.VMEM)
    hbm = pl.BlockSpec(memory_space=pltpu.HBM)
    V = pltpu.VMEM
    mis, dual, lim, norms, tot = pl.pallas_call(
        functools.partial(body, groups, ranks),
        out_shape=(
            jax.ShapeDtypeStruct((scen, 2, nb), f32),
            jax.ShapeDtypeStruct((scen, nb), f32),
            jax.ShapeDtypeStruct((scen, nl), f32),
            jax.ShapeDtypeStruct((scen, 4), f32),
            jax.ShapeDtypeStruct((1, 4), f32),
        ),
        in_specs=[hbm] * 15,
        out_specs=(vmem,) * 5,
        scratch_shapes=[
            V((1, block), f32), V((1, block), f32),
            V((scen, 2, nb), f32), V((scen, 2, nb), f32), V((scen, 2, nb), f32),
            V((scen, nb), f32), V((scen, nl), i32), V((scen, nl), f32), V((scen, nl), f32), V((rows, LANES), f32),
            V((scen, rows, LANES), i32), V((scen, rows, LANES), f32), V((scen, btiles, LANES), f32), V((scen, 1, LANES), f32),
            V((ranks, 2, rows, LANES), i32), V((ranks, 3, rows, LANES), f32), V((ranks, rows, LANES), i32),
            V((ranks, 2, nb), f32), V((ranks, 2, nb), f32), V((ranks, 2, LANES), f32), V((groups, SUB, LANES), f32),
            V((ranks, 2, nb), f32), V((ranks, rows, LANES), f32), V((ranks, btiles, LANES), f32), V((ranks, 1, LANES), f32),
            V((4, tiles, LANES), f32), V((2, ranks * rows, LANES), i32), V((3, ranks * rows, LANES), f32),
            V((ranks * rows, LANES), i32), V((ranks * rows, LANES), f32), V((ranks * rows, LANES), f32), V((6 * high, SPAN), f32),
            V((ranks, 2, nb), f32), V((ranks, btiles, LANES), f32), V((ranks, rows, LANES), f32),
            V((ranks, 2, nb), f32), V((ranks, btiles, LANES), f32), V((ranks, rows, LANES), f32),
            V((ranks, 1, LANES), f32), V((groups, 1, LANES), f32),
            pltpu.SemaphoreType.DMA((15,)),
            pltpu.SemaphoreType.DMA((KINDS,)),
            pltpu.SemaphoreType.DMA((KINDS,)),
        ],
        compiler_params=pltpu.CompilerParams(
            collective_id=0, has_side_effects=True, vmem_limit_bytes=40 << 20
        ),
    )(*(pltpu.with_memory_space_constraint(x, pltpu.HBM) for x in (
        base_vm[None, :], base_va[None, :], delta_state, multipliers, net_inj, ang_grad,
        *(x.reshape(rows, LANES) for x in (from_bus, to_bus, conduct, suscept, charging, rating)),
        status, slack, zdual,
    )))
    return (mis, dual, lim, norms, tot[0])


def solution(mesh):
    placed = (
        P(("ctg", "br")), P(("ctg", "br")),
        P("ctg", None, "br"), P("ctg", None, "br"), P("ctg", None, "br"), P("ctg", "br"),
        P("br"), P("br"), P("ctg", "br"), P("br"), P("br"), P("br"), P("br"),
        P("ctg", "br"), P("ctg", "br"),
    )
    return jax.shard_map(
        per_device,
        mesh=mesh,
        in_specs=placed,
        out_specs=(P("ctg", None, "br"), P("ctg", "br"), P("ctg", "br"), P("ctg", None), P()),
        check_vma=False,
    )
```

```python
import functools

import jax
import jax.numpy as jnp
from jax import lax
from jax.experimental import pallas as pl
from jax.experimental.pallas import tpu as pltpu
from jax.sharding import PartitionSpec as P

LANES = 128
SUB = 8
SPAN = 256
MESH = pl.DeviceIdType.MESH

ENDS, PARAMS, STATUS, MULT, DELTA, PIECE, BASE, NET, WORK, ANG, COMP, ENDS2, PARAMS2, SQ, MIS, DUAL, LIM, TOTAL = range(18)
KINDS = 18


def sin_cos(x):
    y = x * x
    sin_c = (1 / 6227020800, -1 / 39916800, 1 / 362880, -1 / 5040, 1 / 120, -1 / 6)
    cos_c = (-1 / 87178291200, 1 / 479001600, -1 / 3628800, 1 / 40320, -1 / 720, 1 / 24, -0.5)
    s = jnp.full_like(y, sin_c[0])
    for c in sin_c[1:]:
        s = s * y + c
    k = jnp.full_like(y, cos_c[0])
    for c in cos_c[1:]:
        k = k * y + c
    return x + x * y * s, 1.0 + y * k


def body(
    groups, ranks,
    vm_any, va_any, delta_any, mult_any, net_any, ang_any, from_any, to_any,
    g_any, b_any, h_any, rating_any, status_any, slack_any, zdual_any,
    min_, din, lin, norm_out, tot_out,
    vm1, va1, dstg, mstg, nstg, ang8, st8, sl8, zd8, rate,
    ststg, wstg, astg, cstg,
    ebuf, pbuf0, pbuf1, stbuf, mbuf, dbuf, zbuf, cbuf, nbuf, wbuf, abuf, compbuf,
    table, dends, dpar, dst, dmult, dlim, hot, acc,
    mout, dout, lout, sqbuf, rowbuf,
    local, send, recv,
):
    grp, me = lax.axis_index("ctg"), lax.axis_index("br")
    core = lax.rem(grp, 2)
    sibling = grp + 1 - 2 * core
    scen, _, nb = delta_any.shape
    rows = from_any.shape[0]
    btiles = nb // LANES
    tiles = table.shape[1]
    f32, bf16 = jnp.float32, jnp.bfloat16
    piece_len = vm_any.shape[1]

    def fetch(i, src, dst):
        copy = pltpu.make_async_copy(src, dst, local.at[i])
        copy.start()
        return copy

    ends_in = [pltpu.make_async_copy(src, ebuf.at[i, me], local.at[2 + i]) for i, src in enumerate((from_any, to_any))]
    params_in = [
        pltpu.make_async_copy(src, dst, local.at[8 + i])
        for i, (src, dst) in enumerate(((g_any, pbuf0.at[me, 0]), (h_any, pbuf0.at[me, 1]), (b_any, pbuf1.at[me, 0])))
    ]

    @pl.when(core == 0)
    def _():
        for copy in (ends_in[0], params_in[0], params_in[1]):
            copy.start()

    @pl.when(core == 1)
    def _():
        for copy in (ends_in[1], params_in[2]):
            copy.start()

    base_in = [fetch(0, vm_any, vm1), fetch(1, va_any, va1)]
    status_in = [fetch(4, status_any, st8), fetch(5, slack_any, sl8), fetch(6, zdual_any, zd8), fetch(7, rating_any, rate)]
    bus_in = [fetch(11, delta_any, dstg), fetch(12, mult_any, mstg)]
    late_in = [fetch(13, net_any, nstg), fetch(14, ang_any, ang8)]

    barrier = pltpu.get_barrier_semaphore()

    def greet_near(i, carry):
        pl.semaphore_signal(barrier, inc=1, device_id=(grp, lax.rem(me + i, ranks)), device_id_type=MESH)
        return carry

    def greet_far(i, carry):
        pl.semaphore_signal(barrier, inc=1, device_id=(lax.rem(grp + i, groups), me), device_id_type=MESH)
        return carry

    lax.fori_loop(1, ranks, greet_near, 0)
    lax.fori_loop(1, groups, greet_far, 0)

    for copy in base_in + status_in:
        copy.wait()

    lane = lax.broadcasted_iota(jnp.int32, (SUB, LANES), 1)
    pad = jnp.zeros((1, LANES - piece_len), f32)
    piece = jnp.concatenate(
        [jnp.concatenate([vm1[...], pad], axis=1), jnp.concatenate([va1[...], pad], axis=1), jnp.zeros((SUB - 2, LANES), f32)],
        axis=0,
    )
    shift = lax.rem(grp * (ranks * piece_len) + me * piece_len, LANES)
    piece = pltpu.roll(piece, shift, 1)
    zbuf[me] = piece[0:2, :]

    for r in range(rows):
        cols = slice(r * LANES, (r + 1) * LANES)
        ststg[:, r, :] = st8[:, cols]
        wstg[:, r, :] = sl8[:, cols]
    squared = rate[...] * rate[...]
    for s in range(scen):
        wstg[s] = wstg[s] - squared
    comp = st8[...].astype(f32) * (zd8[...] * sl8[...] - 0.01)
    cstg[:, 0, :] = jnp.broadcast_to(jnp.sum(comp * comp, axis=1, keepdims=True), (scen, LANES))

    for copy in bus_in + late_in:
        copy.wait()
    for k in range(btiles):
        astg[:, k, :] = ang8[:, k * LANES : (k + 1) * LANES]

    pl.semaphore_wait(barrier, ranks - 1 + groups - 1)

    def near(kind, step, src, dst):
        pltpu.make_async_remote_copy(
            src_ref=src, dst_ref=dst, send_sem=send.at[kind], recv_sem=recv.at[kind],
            device_id=(grp, lax.rem(me + step, ranks)), device_id_type=MESH,
        ).start()

    def far(kind, step, src, dst):
        pltpu.make_async_remote_copy(
            src_ref=src, dst_ref=dst, send_sem=send.at[kind], recv_sem=recv.at[kind],
            device_id=(lax.rem(grp + step, groups), me), device_id_type=MESH,
        ).start()

    def across(kind, ref):
        return pltpu.make_async_remote_copy(
            src_ref=ref, dst_ref=ref, send_sem=send.at[kind], recv_sem=recv.at[kind],
            device_id=(sibling, me), device_id_type=MESH,
        )

    def whole(kind, ref, n):
        part = ref.at[pl.ds(0, n)]
        return pltpu.make_async_remote_copy(
            src_ref=part, dst_ref=part, send_sem=send.at[kind], recv_sem=recv.at[kind],
            device_id=(sibling, me), device_id_type=MESH,
        )

    def to_near(kind, src_of, dst):
        def go(step, carry):
            near(kind, step, src_of(lax.rem(me + step, ranks)), dst)
            return carry
        lax.fori_loop(1, ranks, go, 0)

    def to_far(kind, src, dst):
        def go(step, carry):
            far(kind, step, src, dst)
            return carry
        lax.fori_loop(1, groups, go, 0)

    to_near(PIECE, lambda p: zbuf.at[me], zbuf.at[me])

    @pl.when(core == 0)
    def _():
        ends_in[0].wait()
        to_near(ENDS, lambda p: ebuf.at[0, me], ebuf.at[0, me])

    @pl.when(core == 1)
    def _():
        ends_in[1].wait()
        to_near(ENDS, lambda p: ebuf.at[1, me], ebuf.at[1, me])

    to_near(MULT, lambda p: mstg.at[p], mbuf.at[me])
    to_near(DELTA, lambda p: dstg.at[p], dbuf.at[me])
    to_near(STATUS, lambda p: ststg.at[p], stbuf.at[me])

    @pl.when(core == 0)
    def _():
        params_in[0].wait()
        params_in[1].wait()
        to_near(PARAMS, lambda p: pbuf0.at[me], pbuf0.at[me])

    @pl.when(core == 1)
    def _():
        params_in[2].wait()
        to_near(PARAMS, lambda p: pbuf1.at[me], pbuf1.at[me])

    to_near(COMP, lambda p: cstg.at[p], compbuf.at[me])
    to_near(NET, lambda p: nstg.at[p], nbuf.at[me])
    to_near(WORK, lambda p: wstg.at[p], wbuf.at[me])
    to_near(ANG, lambda p: astg.at[p], abuf.at[me])

    stbuf[me] = ststg[me]
    dbuf[me] = dstg[me]
    mbuf[me] = mstg[me]
    nbuf[me] = nstg[me]
    wbuf[me] = wstg[me]
    abuf[me] = astg[me]
    compbuf[me] = cstg[me]
    acc[...] = jnp.zeros_like(acc)

    whole(PIECE, zbuf, ranks - 1).wait_recv()
    window = (LANES // 2) * core
    for m in range(3):
        off = m * LANES + lane[0:2, :] - window
        found = jnp.zeros((2, LANES), f32)
        for b in range(ranks):
            inside = (off >= b * piece_len) & (off < (b + 1) * piece_len)
            found = jnp.where(inside, zbuf[b], found)
        cbuf[grp, m : m + 1, :] = found[0:1, :]
        cbuf[grp, 3 + m : 4 + m, :] = found[1:2, :]
    cbuf[grp, 6:8, :] = jnp.zeros((2, LANES), f32)
    to_far(BASE, cbuf.at[grp], cbuf.at[grp])

    for c in range(2):
        @pl.when(core == c)
        def _(c=c):
            whole(ENDS, ebuf.at[c], ranks - 1).wait_recv()
            across(ENDS2, ebuf.at[c]).start()
            across(ENDS2, ebuf.at[1 - c]).wait_recv()

    for end in range(2):
        for z in range(ranks):
            dends[end, z * rows : (z + 1) * rows, :] = ebuf[end, z]

    chunks = dends.shape[1] // SUB
    high = acc.shape[0] // 6
    column0 = lax.broadcasted_iota(jnp.int32, (LANES, LANES), 1)
    labels = [(column0 + k * LANES).astype(bf16) for k in range(SPAN // LANES)]
    steps = lax.broadcasted_iota(jnp.int32, (high, LANES), 0).astype(bf16)

    def at_rows(i):
        return pl.ds(pl.multiple_of(i * SUB, SUB), SUB)

    def spread(x, n):
        return jnp.concatenate([jnp.broadcast_to(x, (2 * SUB, LANES)).astype(bf16)] * (n // (2 * SUB)), axis=0)

    def make_hot(i, carry):
        for end in range(2):
            low = dends[end, at_rows(i), :] & (SPAN - 1)
            for r in range(SUB):
                spots = spread(low[r : r + 1, :], LANES).T
                for k, label in enumerate(labels):
                    hot[end, i, k, r * LANES : (r + 1) * LANES, :] = jnp.where(spots == label, bf16(1), bf16(0))
        return carry

    lax.fori_loop(0, chunks, make_hot, 0)

    whole(MULT, mbuf, ranks - 1).wait_recv()
    for z in range(ranks):
        for q in range(2):
            for k in range(btiles):
                at = z * btiles + k
                table[2 + q, at : at + 1, :] = mbuf[z, q : q + 1, k * LANES : (k + 1) * LANES]

    def pick(i, first):
        picked = []
        for end in range(2):
            spot = dends[end, at_rows(i), :]
            low, tile = spot & (LANES - 1), spot >> 7
            found = [jnp.zeros((SUB, LANES), f32) for _ in range(2)]
            for k in range(tiles):
                here = tile == k
                for q in range(2):
                    row = jnp.broadcast_to(table[first + q, k : k + 1, :], (SUB, LANES))
                    got = jnp.take_along_axis(row, low, axis=1, mode="promise_in_bounds")
                    found[q] = jnp.where(here, got, found[q])
            picked += found
        return tuple(picked)

    def keep(i):
        for k, x in enumerate(pick(i, 2)):
            dmult[k, at_rows(i), :] = x

    def keep_two(j, carry):
        keep(2 * j)
        keep(2 * j + 1)
        return carry

    lax.fori_loop(0, chunks // 2, keep_two, 0)
    if chunks % 2:
        keep(chunks - 1)

    whole(STATUS, stbuf, ranks - 1).wait_recv()
    for z in range(ranks):
        dst[z * rows : (z + 1) * rows, :] = stbuf[z]

    @pl.when(core == 0)
    def _():
        whole(PARAMS, pbuf0, ranks - 1).wait_recv()
        across(PARAMS2, pbuf0).start()
        across(PARAMS2, pbuf1).wait_recv()

    @pl.when(core == 1)
    def _():
        whole(PARAMS, pbuf1, ranks - 1).wait_recv()
        across(PARAMS2, pbuf1).start()
        across(PARAMS2, pbuf0).wait_recv()

    for z in range(ranks):
        dpar[0, z * rows : (z + 1) * rows, :] = pbuf0[z, 0]
        dpar[1, z * rows : (z + 1) * rows, :] = pbuf1[z, 0]
        dpar[2, z * rows : (z + 1) * rows, :] = pbuf0[z, 1]

    whole(DELTA, dbuf, ranks - 1).wait_recv()
    whole(BASE, cbuf, groups - 1).wait_recv()

    for r in range(groups // 2):
        for q in range(2):
            def one(c, m):
                return cbuf[2 * r + c, 3 * q + m : 3 * q + m + 1, :]
            five = (one(0, 0), one(0, 1), one(0, 2) + one(1, 0), one(1, 1), one(1, 2))
            for m in range(5):
                at = 5 * r + m
                z, k = at // btiles, at % btiles
                table[q, at : at + 1, :] = five[m] + dbuf[z, q : q + 1, k * LANES : (k + 1) * LANES]

    def scatter(i, picked):
        vf, af, vt, at = picked
        where_ = at_rows(i)
        mpf, mqf, mpt, mqt = (dmult[k, where_, :] for k in range(4))
        sn, cs = sin_cos(af - at)
        g, b, h = dpar[0, where_, :], dpar[1, where_, :], dpar[2, where_, :]
        live = dst[where_, :].astype(f32)
        u = vf * vt
        gc_bs, gc_mbs = g * cs + b * sn, g * cs - b * sn
        gs_bc, gs_mbc = g * sn + b * cs, g * sn - b * cs
        bh = -(b + h)
        pf = live * (g * vf * vf - u * gc_bs)
        qf = live * (bh * vf * vf - u * gs_mbc)
        pt = live * (g * vt * vt - u * gc_mbs)
        qt = live * (bh * vt * vt + u * gs_bc)
        fd = live * u * (mpf * gs_mbc - mqf * gc_bs + mpt * gs_bc + mqt * gc_mbs)
        dlim[where_, :] = pf * pf + qf * qf
        total = None
        for end, terms in ((0, (pf, qf, fd)), (1, (pt, qt, -fd))):
            parts = []
            for value in terms:
                head = value.astype(bf16).astype(f32)
                parts += [head, value - head]
            tile = dends[end, where_, :] >> 8
            lefts = []
            for r in range(SUB):
                row = slice(r, r + 1)
                mask = spread(tile[row, :], high) == steps
                lefts.append(jnp.concatenate(
                    [jnp.where(mask, spread(x[row, :], high), bf16(0)) for x in parts], axis=0
                ))
            right = jnp.concatenate([hot[end, i, k] for k in range(SPAN // LANES)], axis=1)
            dot = lax.dot_general(
                jnp.concatenate(lefts, axis=1), right, (((1,), (0,)), ((), ())), preferred_element_type=f32
            )
            total = dot if total is None else total + dot
        return total

    def two(i):
        return pick(i, 0) + pick(i + 1, 0)

    def scatter_two(i, picked):
        acc[...] += scatter(i, picked[:4]) + scatter(i + 1, picked[4:])

    def advance(j, picked):
        following = two(2 * j + 1)
        scatter_two(2 * j - 1, picked)
        return following

    first = pick(0, 0)
    following = two(1)
    acc[...] += scatter(0, first)
    scatter_two(chunks - 2, lax.fori_loop(1, chunks // 2, advance, following))

    whole(NET, nbuf, ranks - 1).wait_recv()
    whole(WORK, wbuf, ranks - 1).wait_recv()
    whole(ANG, abuf, ranks - 1).wait_recv()
    whole(COMP, compbuf, ranks - 1).wait_recv()

    per = nb // SPAN
    mis_sq = jnp.zeros((1, SPAN), f32)
    dual_sq = jnp.zeros((1, LANES), f32)
    for z in range(ranks):
        for j in range(per):
            t = z * per + j
            cols = slice(j * SPAN, (j + 1) * SPAN)
            for q in range(3):
                top, bottom = (2 * q) * high + t, (2 * q + 1) * high + t
                row = acc[top : top + 1, :] + acc[bottom : bottom + 1, :]
                if q < 2:
                    row = row - nbuf[z, q : q + 1, cols]
                    mout[z, q : q + 1, cols] = row
                    mis_sq = mis_sq + row * row
                else:
                    for half in range(2):
                        k = 2 * j + half
                        one = row[:, half * LANES : (half + 1) * LANES] + abuf[z, k : k + 1, :]
                        dout[z, k : k + 1, :] = one
                        dual_sq = dual_sq + one * one
    lim_sq = jnp.zeros((rows, LANES), f32)
    for z in range(ranks):
        lim = stbuf[z].astype(f32) * (dlim[z * rows : (z + 1) * rows, :] + wbuf[z])
        lout[z] = lim
        lim_sq = lim_sq + lim * lim
    comp_sq = jnp.zeros((1, LANES), f32)
    for z in range(ranks):
        comp_sq = comp_sq + compbuf[z]

    def total_of(x):
        return jnp.sum(jnp.sum(x, axis=0, keepdims=True), axis=1, keepdims=True)

    lane1 = lane[0:1, :]
    squares = jnp.where(
        lane1 == 0, total_of(mis_sq),
        jnp.where(lane1 == 1, total_of(dual_sq), jnp.where(lane1 == 2, total_of(lim_sq), jnp.where(lane1 == 3, comp_sq, 0.0))),
    )
    sqbuf[me] = squares
    to_near(SQ, lambda p: sqbuf.at[me], sqbuf.at[me])
    to_near(MIS, lambda p: mout.at[p], min_.at[me])
    to_near(DUAL, lambda p: dout.at[p], din.at[me])
    to_near(LIM, lambda p: lout.at[p], lin.at[me])
    min_[me] = mout[me]
    din[me] = dout[me]
    lin[me] = lout[me]

    whole(SQ, sqbuf, ranks - 1).wait_recv()
    column = jnp.zeros((1, LANES), f32)
    for z in range(ranks):
        one = sqbuf[z]
        column = column + one
        norm_out[z : z + 1, :] = jnp.sqrt(one)
    rowbuf[grp] = column
    to_far(TOTAL, rowbuf.at[grp], rowbuf.at[grp])

    whole(MIS, min_, ranks - 1).wait_recv()
    whole(DUAL, din, ranks - 1).wait_recv()
    whole(LIM, lin, ranks - 1).wait_recv()

    whole(ENDS, ebuf.at[0], ranks - 1).wait_send()
    across(ENDS2, ebuf.at[0]).wait_send()

    @pl.when(core == 0)
    def _():
        whole(PARAMS, pbuf0, ranks - 1).wait_send()
        across(PARAMS2, pbuf0).wait_send()

    @pl.when(core == 1)
    def _():
        whole(PARAMS, pbuf1, ranks - 1).wait_send()
        across(PARAMS2, pbuf1).wait_send()

    for kind, ref in (
        (PIECE, zbuf), (STATUS, ststg), (DELTA, dstg), (MULT, mstg), (COMP, cstg), (NET, nstg), (WORK, wstg),
        (ANG, astg), (SQ, sqbuf), (MIS, mout), (DUAL, dout), (LIM, lout),
    ):
        whole(kind, ref, ranks - 1).wait_send()
    whole(BASE, cbuf, groups - 1).wait_send()
    whole(TOTAL, rowbuf, groups - 1).wait_send()

    whole(TOTAL, rowbuf, groups - 1).wait_recv()
    everything = jnp.zeros((1, LANES), f32)
    for i in range(groups):
        everything = everything + rowbuf[i]
    tot_out[...] = jnp.sqrt(everything[:, 0:4] / (scen * groups))


def write_out(min_, din, lin, norms, tot, mis_any, dual_any, lim_any, norm_any, tot_any, dual, lim, turned, sems):
    copies = [
        pltpu.make_async_copy(src, dst, sems.at[i])
        for i, (src, dst) in enumerate((
            (min_, mis_any), (tot, tot_any), (dual, dual_any), (lim, lim_any), (turned, norm_any),
        ))
    ]
    copies[0].start()
    copies[1].start()
    for k in range(din.shape[1]):
        dual[:, k * LANES : (k + 1) * LANES] = din[:, k, :]
    copies[2].start()
    for r in range(lin.shape[1]):
        lim[:, r * LANES : (r + 1) * LANES] = lin[:, r, :]
    copies[3].start()
    turned[...] = norms[...].T[0:4, :]
    copies[4].start()
    for copy in copies:
        copy.wait()


def per_device(
    base_vm, base_va, delta_state, multipliers, net_inj, ang_grad, from_bus, to_bus,
    status, conduct, suscept, charging, rating, slack, zdual,
):
    groups, ranks = lax.axis_size("ctg"), lax.axis_size("br")
    scen, _, nb = delta_state.shape
    nl = from_bus.shape[0]
    rows, btiles = nl // LANES, nb // LANES
    buses = nb * ranks
    tiles = buses // LANES
    high = -(-(buses // SPAN) // 16) * 16
    block = base_vm.shape[0]
    f32, i32 = jnp.float32, jnp.int32
    vmem = pl.BlockSpec(memory_space=pltpu.VMEM)
    hbm = pl.BlockSpec(memory_space=pltpu.HBM)
    V = pltpu.VMEM
    outs = pl.pallas_call(
        functools.partial(body, groups, ranks),
        out_shape=(
            jax.ShapeDtypeStruct((ranks, 2, nb), f32),
            jax.ShapeDtypeStruct((ranks, btiles, LANES), f32),
            jax.ShapeDtypeStruct((ranks, rows, LANES), f32),
            jax.ShapeDtypeStruct((scen, LANES), f32),
            jax.ShapeDtypeStruct((1, 4), f32),
        ),
        in_specs=[hbm] * 15,
        out_specs=(vmem,) * 5,
        scratch_shapes=[
            V((1, block), f32), V((1, block), f32),
            V((scen, 2, nb), f32), V((scen, 2, nb), f32), V((scen, 2, nb), f32),
            V((scen, nb), f32), V((scen, nl), i32), V((scen, nl), f32), V((scen, nl), f32), V((rows, LANES), f32),
            V((scen, rows, LANES), i32), V((scen, rows, LANES), f32), V((scen, btiles, LANES), f32), V((scen, 1, LANES), f32),
            V((2, ranks, rows, LANES), i32), V((ranks, 2, rows, LANES), f32), V((ranks, 1, rows, LANES), f32),
            V((ranks, rows, LANES), i32),
            V((ranks, 2, nb), f32), V((ranks, 2, nb), f32), V((ranks, 2, LANES), f32), V((groups, SUB, LANES), f32),
            V((ranks, 2, nb), f32), V((ranks, rows, LANES), f32), V((ranks, btiles, LANES), f32), V((ranks, 1, LANES), f32),
            V((4, tiles, LANES), f32), V((2, ranks * rows, LANES), i32), V((3, ranks * rows, LANES), f32),
            V((ranks * rows, LANES), i32), V((4, ranks * rows, LANES), f32), V((ranks * rows, LANES), f32),
            V((2, ranks * rows // SUB, SPAN // LANES, SUB * LANES, LANES), jnp.bfloat16), V((6 * high, SPAN), f32),
            V((ranks, 2, nb), f32), V((ranks, btiles, LANES), f32), V((ranks, rows, LANES), f32),
            V((ranks, 1, LANES), f32), V((groups, 1, LANES), f32),
            pltpu.SemaphoreType.DMA((15,)),
            pltpu.SemaphoreType.DMA((KINDS,)),
            pltpu.SemaphoreType.DMA((KINDS,)),
        ],
        compiler_params=pltpu.CompilerParams(
            collective_id=0, has_side_effects=True, vmem_limit_bytes=40 << 20
        ),
    )(*(pltpu.with_memory_space_constraint(x, pltpu.HBM) for x in (
        base_vm[None, :], base_va[None, :], delta_state, multipliers, net_inj, ang_grad,
        *(x.reshape(rows, LANES) for x in (from_bus, to_bus, conduct, suscept, charging, rating)),
        status, slack, zdual,
    )))
    mis, dual, lim, norms, tot = pl.pallas_call(
        write_out,
        out_shape=(
            jax.ShapeDtypeStruct((scen, 2, nb), f32),
            jax.ShapeDtypeStruct((scen, nb), f32),
            jax.ShapeDtypeStruct((scen, nl), f32),
            jax.ShapeDtypeStruct((4, scen), f32),
            jax.ShapeDtypeStruct((1, 4), f32),
        ),
        in_specs=[vmem] * 5,
        out_specs=(pl.BlockSpec(memory_space=pl.ANY),) * 5,
        scratch_shapes=[
            V((scen, nb), f32), V((scen, nl), f32), V((4, scen), f32), pltpu.SemaphoreType.DMA((5,)),
        ],
        compiler_params=pltpu.CompilerParams(vmem_limit_bytes=8 << 20),
    )(*outs)
    return (mis, dual, lim, norms.T, tot[0])


def solution(mesh):
    placed = (
        P(("ctg", "br")), P(("ctg", "br")),
        P("ctg", None, "br"), P("ctg", None, "br"), P("ctg", None, "br"), P("ctg", "br"),
        P("br"), P("br"), P("ctg", "br"), P("br"), P("br"), P("br"), P("br"),
        P("ctg", "br"), P("ctg", "br"),
    )
    return jax.shard_map(
        per_device,
        mesh=mesh,
        in_specs=placed,
        out_specs=(P("ctg", None, "br"), P("ctg", "br"), P("ctg", "br"), P("ctg", None), P()),
        check_vma=False,
    )
```

```python
import functools

import jax
import jax.numpy as jnp
from jax import lax
from jax.experimental import pallas as pl
from jax.experimental.pallas import tpu as pltpu
from jax.sharding import PartitionSpec as P

LANES = 128
SUB = 8
SPAN = 256
MESH = pl.DeviceIdType.MESH

ENDS, PARAMS, STATUS, MULT, DELTA, PIECE, BASE, NET, WORK, ANG, COMP, ENDS2, PARAMS2, SQ, MIS, DUAL, LIM, TOTAL = range(18)
KINDS = 18


def sin_cos(x):
    y = x * x
    sin_c = (1 / 6227020800, -1 / 39916800, 1 / 362880, -1 / 5040, 1 / 120, -1 / 6)
    cos_c = (-1 / 87178291200, 1 / 479001600, -1 / 3628800, 1 / 40320, -1 / 720, 1 / 24, -0.5)
    s = jnp.full_like(y, sin_c[0])
    for c in sin_c[1:]:
        s = s * y + c
    k = jnp.full_like(y, cos_c[0])
    for c in cos_c[1:]:
        k = k * y + c
    return x + x * y * s, 1.0 + y * k


def body(
    groups, ranks,
    vm_any, va_any, delta_any, mult_any, net_any, ang_any, from_any, to_any,
    g_any, b_any, h_any, rating_any, status_any, slack_any, zdual_any,
    min_, din, lin, norm_out, tot_out,
    vm1, va1, dstg, mstg, nstg, ang8, st8, sl8, zd8, rate,
    ststg, wstg, astg, cstg,
    pstg, pown, pz, pall, ebuf, stbuf, mbuf, dbuf, zbuf, cbuf, nbuf, wbuf, abuf, compbuf,
    table, dends, dpar, dst, dmult, dlim, hot, acc,
    mout, dout, lout, sqbuf, rowbuf,
    local, send, recv, ends_recv, ends_recv2,
):
    grp, me = lax.axis_index("ctg"), lax.axis_index("br")
    core = lax.rem(grp, 2)
    shares = pown.shape[0]
    line = lax.rem(grp, groups // (shares // 2)) - core
    part = 2 * (grp // (groups // (shares // 2))) + core
    sibling = grp + 1 - 2 * core
    scen, _, nb = delta_any.shape
    rows = from_any.shape[0]
    btiles = nb // LANES
    tiles = table.shape[1]
    f32, bf16 = jnp.float32, jnp.bfloat16
    piece_len = vm_any.shape[1]

    def fetch(i, src, dst):
        copy = pltpu.make_async_copy(src, dst, local.at[i])
        copy.start()
        return copy

    ends_in = [fetch(2, from_any, ebuf.at[0, me]), fetch(3, to_any, ebuf.at[1, me])]
    base_in = [fetch(0, vm_any, vm1), fetch(1, va_any, va1)]
    status_in = [fetch(4, status_any, st8), fetch(5, slack_any, sl8), fetch(6, zdual_any, zd8), fetch(7, rating_any, rate)]
    params_in = [fetch(8, g_any, pstg.at[0]), fetch(9, b_any, pstg.at[1]), fetch(10, h_any, pstg.at[2])]
    bus_in = [fetch(11, delta_any, dstg), fetch(12, mult_any, mstg)]
    late_in = [fetch(13, net_any, nstg), fetch(14, ang_any, ang8)]

    barrier = pltpu.get_barrier_semaphore()

    def greet_near(i, carry):
        pl.semaphore_signal(barrier, inc=1, device_id=(grp, lax.rem(me + i, ranks)), device_id_type=MESH)
        return carry

    def greet_far(i, carry):
        pl.semaphore_signal(barrier, inc=1, device_id=(lax.rem(grp + i, groups), me), device_id_type=MESH)
        return carry

    lax.fori_loop(1, ranks, greet_near, 0)
    lax.fori_loop(1, groups, greet_far, 0)

    for copy in base_in + status_in:
        copy.wait()

    lane = lax.broadcasted_iota(jnp.int32, (SUB, LANES), 1)
    pad = jnp.zeros((1, LANES - piece_len), f32)
    piece = jnp.concatenate(
        [jnp.concatenate([vm1[...], pad], axis=1), jnp.concatenate([va1[...], pad], axis=1), jnp.zeros((SUB - 2, LANES), f32)],
        axis=0,
    )
    shift = lax.rem(grp * (ranks * piece_len) + me * piece_len, LANES)
    piece = pltpu.roll(piece, shift, 1)
    zbuf[me] = piece[0:2, :]

    for r in range(rows):
        cols = slice(r * LANES, (r + 1) * LANES)
        ststg[:, r, :] = st8[:, cols]
        wstg[:, r, :] = sl8[:, cols]
    squared = rate[...] * rate[...]
    for s in range(scen):
        wstg[s] = wstg[s] - squared
    comp = st8[...].astype(f32) * (zd8[...] * sl8[...] - 0.01)
    cstg[:, 0, :] = jnp.broadcast_to(jnp.sum(comp * comp, axis=1, keepdims=True), (scen, LANES))

    for copy in ends_in + params_in + bus_in + late_in:
        copy.wait()
    share = pown.shape[1]
    for j in range(3 * rows):
        q, r = j // rows, j % rows
        pown[j // share, j % share : j % share + 1, :] = pstg[q, r : r + 1, :]
    for j in range(3 * rows, pown.shape[0] * share):
        pown[j // share, j % share : j % share + 1, :] = jnp.zeros((1, LANES), f32)
    for k in range(btiles):
        astg[:, k, :] = ang8[:, k * LANES : (k + 1) * LANES]

    pl.semaphore_wait(barrier, ranks - 1 + groups - 1)

    def near(kind, step, src, dst):
        pltpu.make_async_remote_copy(
            src_ref=src, dst_ref=dst, send_sem=send.at[kind], recv_sem=recv.at[kind],
            device_id=(grp, lax.rem(me + step, ranks)), device_id_type=MESH,
        ).start()

    def far(kind, step, src, dst):
        pltpu.make_async_remote_copy(
            src_ref=src, dst_ref=dst, send_sem=send.at[kind], recv_sem=recv.at[kind],
            device_id=(lax.rem(grp + step, groups), me), device_id_type=MESH,
        ).start()

    def whole(kind, ref, n):
        part = ref.at[pl.ds(0, n)]
        return pltpu.make_async_remote_copy(
            src_ref=part, dst_ref=part, send_sem=send.at[kind], recv_sem=recv.at[kind],
            device_id=(sibling, me), device_id_type=MESH,
        )

    def to_near(kind, src_of, dst):
        def go(step, carry):
            near(kind, step, src_of(lax.rem(me + step, ranks)), dst)
            return carry
        lax.fori_loop(1, ranks, go, 0)

    def to_far(kind, src, dst):
        def go(step, carry):
            far(kind, step, src, dst)
            return carry
        lax.fori_loop(1, groups, go, 0)

    to_near(PIECE, lambda p: zbuf.at[me], zbuf.at[me])

    def send_ends(step, carry):
        pltpu.make_async_remote_copy(
            src_ref=ebuf.at[core, me], dst_ref=ebuf.at[core, me], send_sem=send.at[ENDS], recv_sem=ends_recv.at[ranks - step],
            device_id=(grp, lax.rem(me + step, ranks)), device_id_type=MESH,
        ).start()
        return carry

    lax.fori_loop(1, ranks, send_ends, 0)
    to_near(PARAMS, lambda p: pown.at[part], pz.at[me])
    to_near(MULT, lambda p: mstg.at[p], mbuf.at[me])
    to_near(DELTA, lambda p: dstg.at[p], dbuf.at[me])
    to_near(STATUS, lambda p: ststg.at[p], stbuf.at[me])
    to_near(COMP, lambda p: cstg.at[p], compbuf.at[me])
    to_near(NET, lambda p: nstg.at[p], nbuf.at[me])
    to_near(WORK, lambda p: wstg.at[p], wbuf.at[me])
    to_near(ANG, lambda p: astg.at[p], abuf.at[me])

    pz[me] = pown[part]
    stbuf[me] = ststg[me]
    dbuf[me] = dstg[me]
    mbuf[me] = mstg[me]
    nbuf[me] = nstg[me]
    wbuf[me] = wstg[me]
    abuf[me] = astg[me]
    compbuf[me] = cstg[me]
    acc[...] = jnp.zeros_like(acc)

    source = [lax.rem(me + j, ranks) for j in range(ranks)]
    chunks = dends.shape[1] // SUB
    high = acc.shape[0] // 6
    column0 = lax.broadcasted_iota(jnp.int32, (LANES, LANES), 1)
    labels = [(column0 + k * LANES).astype(bf16) for k in range(SPAN // LANES)]
    steps = lax.broadcasted_iota(jnp.int32, (high, LANES), 0).astype(bf16)

    def at_rows(i):
        return pl.ds(pl.multiple_of(i * SUB, SUB), SUB)

    def spread(x, n):
        return jnp.concatenate([jnp.broadcast_to(x, (2 * SUB, LANES)).astype(bf16)] * (n // (2 * SUB)), axis=0)

    def make_hot(step):
        origin = lax.rem(me + step, ranks)
        for end in range(2):
            low = ebuf[end, origin] & (SPAN - 1)
            for r in range(rows):
                spots = spread(low[r : r + 1, :], LANES).T
                place = pl.ds(pl.multiple_of((step * rows + r) * LANES, LANES), LANES)
                for k, label in enumerate(labels):
                    hot[end, k, place, :] = jnp.where(spots == label, bf16(1), bf16(0))

    def ends_copy(sems, half, origin, step):
        return pltpu.make_async_remote_copy(
            src_ref=ebuf.at[half, origin], dst_ref=ebuf.at[half, origin], send_sem=send.at[ENDS2], recv_sem=sems.at[step],
            device_id=(sibling, me), device_id_type=MESH,
        )

    make_hot(0)

    def turn(t):
        return jnp.where(lax.rem(t, 2) == 1, (t + 1) // 2, ranks - t // 2)

    def forward(t, carry):
        step = turn(t)
        origin = lax.rem(me + step, ranks)
        ends_copy(ends_recv, core, origin, step).wait_recv()
        ends_copy(ends_recv2, core, origin, step).start()
        return carry

    lax.fori_loop(1, ranks, forward, 0)

    whole(PIECE, zbuf, ranks - 1).wait_recv()
    window = (LANES // 2) * core
    for m in range(3):
        off = m * LANES + lane[0:2, :] - window
        found = jnp.zeros((2, LANES), f32)
        for b in range(ranks):
            inside = (off >= b * piece_len) & (off < (b + 1) * piece_len)
            found = jnp.where(inside, zbuf[b], found)
        cbuf[grp, m : m + 1, :] = found[0:1, :]
        cbuf[grp, 3 + m : 4 + m, :] = found[1:2, :]
    cbuf[grp, 6:8, :] = jnp.zeros((2, LANES), f32)
    to_far(BASE, cbuf.at[grp], cbuf.at[grp])

    def arrive(t, carry):
        step = turn(t)
        ends_copy(ends_recv2, 1 - core, lax.rem(me + step, ranks), step).wait_recv()
        make_hot(step)
        return carry

    lax.fori_loop(1, ranks, arrive, 0)
    for end in range(2):
        for j in range(ranks):
            dends[end, j * rows : (j + 1) * rows, :] = ebuf[end, source[j]]

    whole(PARAMS, pz, ranks - 1).wait_recv()
    pall[part] = pz[...]

    def share_params(d, carry):
        other = lax.rem(part + d, shares)
        pltpu.make_async_remote_copy(
            src_ref=pz, dst_ref=pall.at[part], send_sem=send.at[PARAMS2], recv_sem=recv.at[PARAMS2],
            device_id=((other // 2) * (groups // (shares // 2)) + line + lax.rem(other, 2), me), device_id_type=MESH,
        ).start()
        return carry

    lax.fori_loop(1, shares, share_params, 0)

    whole(MULT, mbuf, ranks - 1).wait_recv()
    for z in range(ranks):
        for q in range(2):
            for k in range(btiles):
                at = z * btiles + k
                table[2 + q, at : at + 1, :] = mbuf[z, q : q + 1, k * LANES : (k + 1) * LANES]

    def pick(i, first):
        picked = []
        for end in range(2):
            spot = dends[end, at_rows(i), :]
            low, tile = spot & (LANES - 1), spot >> 7
            found = [jnp.zeros((SUB, LANES), f32) for _ in range(2)]
            for k in range(tiles):
                here = tile == k
                for q in range(2):
                    row = jnp.broadcast_to(table[first + q, k : k + 1, :], (SUB, LANES))
                    got = jnp.take_along_axis(row, low, axis=1, mode="promise_in_bounds")
                    found[q] = jnp.where(here, got, found[q])
            picked += found
        return tuple(picked)

    def keep(i):
        for k, x in enumerate(pick(i, 2)):
            dmult[k, at_rows(i), :] = x

    def keep_two(j, carry):
        keep(2 * j)
        keep(2 * j + 1)
        return carry

    lax.fori_loop(0, chunks // 2, keep_two, 0)
    if chunks % 2:
        keep(chunks - 1)

    whole(STATUS, stbuf, ranks - 1).wait_recv()
    for j in range(ranks):
        dst[j * rows : (j + 1) * rows, :] = stbuf[source[j]]

    whole(PARAMS2, pall, shares - 1).wait_recv()
    for j in range(ranks):
        for k in range(3 * rows):
            q, r = k // rows, j * rows + k % rows
            dpar[q, r : r + 1, :] = pall[k // share, source[j], k % share : k % share + 1, :]

    whole(DELTA, dbuf, ranks - 1).wait_recv()
    whole(BASE, cbuf, groups - 1).wait_recv()

    for r in range(groups // 2):
        for q in range(2):
            def one(c, m):
                return cbuf[2 * r + c, 3 * q + m : 3 * q + m + 1, :]
            five = (one(0, 0), one(0, 1), one(0, 2) + one(1, 0), one(1, 1), one(1, 2))
            for m in range(5):
                at = 5 * r + m
                z, k = at // btiles, at % btiles
                table[q, at : at + 1, :] = five[m] + dbuf[z, q : q + 1, k * LANES : (k + 1) * LANES]

    def scatter(i, picked):
        vf, af, vt, at = picked
        where_ = at_rows(i)
        mpf, mqf, mpt, mqt = (dmult[k, where_, :] for k in range(4))
        sn, cs = sin_cos(af - at)
        g, b, h = dpar[0, where_, :], dpar[1, where_, :], dpar[2, where_, :]
        live = dst[where_, :].astype(f32)
        u = vf * vt
        gc_bs, gc_mbs = g * cs + b * sn, g * cs - b * sn
        gs_bc, gs_mbc = g * sn + b * cs, g * sn - b * cs
        bh = -(b + h)
        pf = live * (g * vf * vf - u * gc_bs)
        qf = live * (bh * vf * vf - u * gs_mbc)
        pt = live * (g * vt * vt - u * gc_mbs)
        qt = live * (bh * vt * vt + u * gs_bc)
        fd = live * u * (mpf * gs_mbc - mqf * gc_bs + mpt * gs_bc + mqt * gc_mbs)
        dlim[where_, :] = pf * pf + qf * qf
        total = None
        for end, terms in ((0, (pf, qf, fd)), (1, (pt, qt, -fd))):
            parts = []
            for value in terms:
                head = value.astype(bf16).astype(f32)
                parts += [head, value - head]
            tile = dends[end, where_, :] >> 8
            lefts = []
            for r in range(SUB):
                row = slice(r, r + 1)
                mask = spread(tile[row, :], high) == steps
                lefts.append(jnp.concatenate(
                    [jnp.where(mask, spread(x[row, :], high), bf16(0)) for x in parts], axis=0
                ))
            spots = pl.ds(pl.multiple_of(i * (SUB * LANES), SUB * LANES), SUB * LANES)
            right = jnp.concatenate([hot[end, k, spots, :] for k in range(SPAN // LANES)], axis=1)
            dot = lax.dot_general(
                jnp.concatenate(lefts, axis=1), right, (((1,), (0,)), ((), ())), preferred_element_type=f32
            )
            total = dot if total is None else total + dot
        return total

    def two(i):
        return pick(i, 0) + pick(i + 1, 0)

    def scatter_two(i, picked):
        acc[...] += scatter(i, picked[:4]) + scatter(i + 1, picked[4:])

    def advance(j, picked):
        following = two(2 * j + 1)
        scatter_two(2 * j - 1, picked)
        return following

    first = pick(0, 0)
    following = two(1)
    acc[...] += scatter(0, first)
    scatter_two(chunks - 2, lax.fori_loop(1, chunks // 2, advance, following))

    whole(NET, nbuf, ranks - 1).wait_recv()
    whole(WORK, wbuf, ranks - 1).wait_recv()
    whole(ANG, abuf, ranks - 1).wait_recv()
    whole(COMP, compbuf, ranks - 1).wait_recv()

    per = nb // SPAN
    mis_sq = jnp.zeros((1, SPAN), f32)
    dual_sq = jnp.zeros((1, LANES), f32)
    for z in range(ranks):
        for j in range(per):
            t = z * per + j
            cols = slice(j * SPAN, (j + 1) * SPAN)
            for q in range(3):
                top, bottom = (2 * q) * high + t, (2 * q + 1) * high + t
                row = acc[top : top + 1, :] + acc[bottom : bottom + 1, :]
                if q < 2:
                    row = row - nbuf[z, q : q + 1, cols]
                    mout[z, q : q + 1, cols] = row
                    mis_sq = mis_sq + row * row
                else:
                    for half in range(2):
                        k = 2 * j + half
                        one = row[:, half * LANES : (half + 1) * LANES] + abuf[z, k : k + 1, :]
                        dout[z, k : k + 1, :] = one
                        dual_sq = dual_sq + one * one
    lim_sq = jnp.zeros((rows, LANES), f32)
    for j in range(ranks):
        z = source[j]
        lim = stbuf[z].astype(f32) * (dlim[j * rows : (j + 1) * rows, :] + wbuf[z])
        lout[z] = lim
        lim_sq = lim_sq + lim * lim
    comp_sq = jnp.zeros((1, LANES), f32)
    for z in range(ranks):
        comp_sq = comp_sq + compbuf[z]

    def total_of(x):
        return jnp.sum(jnp.sum(x, axis=0, keepdims=True), axis=1, keepdims=True)

    lane1 = lane[0:1, :]
    squares = jnp.where(
        lane1 == 0, total_of(mis_sq),
        jnp.where(lane1 == 1, total_of(dual_sq), jnp.where(lane1 == 2, total_of(lim_sq), jnp.where(lane1 == 3, comp_sq, 0.0))),
    )
    sqbuf[me] = squares
    to_near(SQ, lambda p: sqbuf.at[me], sqbuf.at[me])
    to_near(MIS, lambda p: mout.at[p], min_.at[me])
    to_near(DUAL, lambda p: dout.at[p], din.at[me])
    to_near(LIM, lambda p: lout.at[p], lin.at[me])
    min_[me] = mout[me]
    din[me] = dout[me]
    lin[me] = lout[me]

    whole(SQ, sqbuf, ranks - 1).wait_recv()
    column = jnp.zeros((1, LANES), f32)
    for z in range(ranks):
        one = sqbuf[z]
        column = column + one
        norm_out[z : z + 1, :] = jnp.sqrt(one)
    rowbuf[grp] = column
    to_far(TOTAL, rowbuf.at[grp], rowbuf.at[grp])

    whole(MIS, min_, ranks - 1).wait_recv()
    whole(DUAL, din, ranks - 1).wait_recv()
    whole(LIM, lin, ranks - 1).wait_recv()

    whole(ENDS, ebuf.at[0], ranks - 1).wait_send()
    whole(ENDS2, ebuf.at[0], ranks - 1).wait_send()
    whole(PARAMS, pown, ranks - 1).wait_send()
    whole(PARAMS2, pall, shares - 1).wait_send()
    for kind, ref in (
        (PIECE, zbuf), (STATUS, ststg), (DELTA, dstg), (MULT, mstg), (COMP, cstg), (NET, nstg), (WORK, wstg),
        (ANG, astg), (SQ, sqbuf), (MIS, mout), (DUAL, dout), (LIM, lout),
    ):
        whole(kind, ref, ranks - 1).wait_send()
    whole(BASE, cbuf, groups - 1).wait_send()
    whole(TOTAL, rowbuf, groups - 1).wait_send()

    whole(TOTAL, rowbuf, groups - 1).wait_recv()
    everything = jnp.zeros((1, LANES), f32)
    for i in range(groups):
        everything = everything + rowbuf[i]
    tot_out[...] = jnp.sqrt(everything[:, 0:4] / (scen * groups))


def write_out(min_, din, lin, norms, tot, mis_any, dual_any, lim_any, norm_any, tot_any, dual, lim, turned, sems):
    copies = [
        pltpu.make_async_copy(src, dst, sems.at[i])
        for i, (src, dst) in enumerate((
            (min_, mis_any), (tot, tot_any), (dual, dual_any), (lim, lim_any), (turned, norm_any),
        ))
    ]
    copies[0].start()
    copies[1].start()
    for k in range(din.shape[1]):
        dual[:, k * LANES : (k + 1) * LANES] = din[:, k, :]
    copies[2].start()
    for r in range(lin.shape[1]):
        lim[:, r * LANES : (r + 1) * LANES] = lin[:, r, :]
    copies[3].start()
    turned[...] = norms[...].T[0:4, :]
    copies[4].start()
    for copy in copies:
        copy.wait()


def per_device(
    base_vm, base_va, delta_state, multipliers, net_inj, ang_grad, from_bus, to_bus,
    status, conduct, suscept, charging, rating, slack, zdual,
):
    groups, ranks = lax.axis_size("ctg"), lax.axis_size("br")
    scen, _, nb = delta_state.shape
    nl = from_bus.shape[0]
    rows, btiles = nl // LANES, nb // LANES
    buses = nb * ranks
    tiles = buses // LANES
    high = -(-(buses // SPAN) // 16) * 16
    block = base_vm.shape[0]
    shares = 8
    share = -(-3 * rows // shares)
    f32, i32 = jnp.float32, jnp.int32
    vmem = pl.BlockSpec(memory_space=pltpu.VMEM)
    hbm = pl.BlockSpec(memory_space=pltpu.HBM)
    V = pltpu.VMEM
    outs = pl.pallas_call(
        functools.partial(body, groups, ranks),
        out_shape=(
            jax.ShapeDtypeStruct((ranks, 2, nb), f32),
            jax.ShapeDtypeStruct((ranks, btiles, LANES), f32),
            jax.ShapeDtypeStruct((ranks, rows, LANES), f32),
            jax.ShapeDtypeStruct((scen, LANES), f32),
            jax.ShapeDtypeStruct((1, 4), f32),
        ),
        in_specs=[hbm] * 15,
        out_specs=(vmem,) * 5,
        scratch_shapes=[
            V((1, block), f32), V((1, block), f32),
            V((scen, 2, nb), f32), V((scen, 2, nb), f32), V((scen, 2, nb), f32),
            V((scen, nb), f32), V((scen, nl), i32), V((scen, nl), f32), V((scen, nl), f32), V((rows, LANES), f32),
            V((scen, rows, LANES), i32), V((scen, rows, LANES), f32), V((scen, btiles, LANES), f32), V((scen, 1, LANES), f32),
            V((3, rows, LANES), f32), V((shares, share, LANES), f32), V((ranks, share, LANES), f32),
            V((shares, ranks, share, LANES), f32), V((2, ranks, rows, LANES), i32),
            V((ranks, rows, LANES), i32),
            V((ranks, 2, nb), f32), V((ranks, 2, nb), f32), V((ranks, 2, LANES), f32), V((groups, SUB, LANES), f32),
            V((ranks, 2, nb), f32), V((ranks, rows, LANES), f32), V((ranks, btiles, LANES), f32), V((ranks, 1, LANES), f32),
            V((4, tiles, LANES), f32), V((2, ranks * rows, LANES), i32), V((3, ranks * rows, LANES), f32),
            V((ranks * rows, LANES), i32), V((4, ranks * rows, LANES), f32), V((ranks * rows, LANES), f32),
            V((2, SPAN // LANES, ranks * nl, LANES), jnp.bfloat16), V((6 * high, SPAN), f32),
            V((ranks, 2, nb), f32), V((ranks, btiles, LANES), f32), V((ranks, rows, LANES), f32),
            V((ranks, 1, LANES), f32), V((groups, 1, LANES), f32),
            pltpu.SemaphoreType.DMA((15,)),
            pltpu.SemaphoreType.DMA((KINDS,)),
            pltpu.SemaphoreType.DMA((KINDS,)),
            pltpu.SemaphoreType.DMA((ranks,)),
            pltpu.SemaphoreType.DMA((ranks,)),
        ],
        compiler_params=pltpu.CompilerParams(
            collective_id=0, has_side_effects=True, vmem_limit_bytes=40 << 20
        ),
    )(*(pltpu.with_memory_space_constraint(x, pltpu.HBM) for x in (
        base_vm[None, :], base_va[None, :], delta_state, multipliers, net_inj, ang_grad,
        *(x.reshape(rows, LANES) for x in (from_bus, to_bus, conduct, suscept, charging, rating)),
        status, slack, zdual,
    )))
    mis, dual, lim, norms, tot = pl.pallas_call(
        write_out,
        out_shape=(
            jax.ShapeDtypeStruct((scen, 2, nb), f32),
            jax.ShapeDtypeStruct((scen, nb), f32),
            jax.ShapeDtypeStruct((scen, nl), f32),
            jax.ShapeDtypeStruct((4, scen), f32),
            jax.ShapeDtypeStruct((1, 4), f32),
        ),
        in_specs=[vmem] * 5,
        out_specs=(pl.BlockSpec(memory_space=pl.ANY),) * 5,
        scratch_shapes=[
            V((scen, nb), f32), V((scen, nl), f32), V((4, scen), f32), pltpu.SemaphoreType.DMA((5,)),
        ],
        compiler_params=pltpu.CompilerParams(vmem_limit_bytes=8 << 20),
    )(*outs)
    return (mis, dual, lim, norms.T, tot[0])


def solution(mesh):
    placed = (
        P(("ctg", "br")), P(("ctg", "br")),
        P("ctg", None, "br"), P("ctg", None, "br"), P("ctg", None, "br"), P("ctg", "br"),
        P("br"), P("br"), P("ctg", "br"), P("br"), P("br"), P("br"), P("br"),
        P("ctg", "br"), P("ctg", "br"),
    )
    return jax.shard_map(
        per_device,
        mesh=mesh,
        in_specs=placed,
        out_specs=(P("ctg", None, "br"), P("ctg", "br"), P("ctg", "br"), P("ctg", None), P()),
        check_vma=False,
    )
```

```python
import functools

import jax
import jax.numpy as jnp
from jax import lax
from jax.experimental import pallas as pl
from jax.experimental.pallas import tpu as pltpu
from jax.sharding import PartitionSpec as P

LANES = 128
SUB = 8
SPAN = 256
MESH = pl.DeviceIdType.MESH

ENDS, PARAMS, STATUS, MULT, DELTA, PIECE, BASE, NET, WORK, ANG, COMP, ENDS2, PARAMS2, SQ, MIS, DUAL, LIM, TOTAL = range(18)
KINDS = 18


def sin_cos(x):
    y = x * x
    sin_c = (1 / 6227020800, -1 / 39916800, 1 / 362880, -1 / 5040, 1 / 120, -1 / 6)
    cos_c = (-1 / 87178291200, 1 / 479001600, -1 / 3628800, 1 / 40320, -1 / 720, 1 / 24, -0.5)
    s = jnp.full_like(y, sin_c[0])
    for c in sin_c[1:]:
        s = s * y + c
    k = jnp.full_like(y, cos_c[0])
    for c in cos_c[1:]:
        k = k * y + c
    return x + x * y * s, 1.0 + y * k


def body(
    groups, ranks,
    vm_any, va_any, delta_any, mult_any, net_any, ang_any, from_any, to_any,
    g_any, b_any, h_any, rating_any, status_any, slack_any, zdual_any,
    min_, din, lin, norm_out, tot_out,
    vm1, va1, dstg, mstg, nstg, ang8, st8, sl8, zd8, rate,
    ststg, wstg, astg, cstg,
    pstg, pown, pz, pall, ebuf, stbuf, mbuf, dbuf, zbuf, cbuf, nbuf, wbuf, abuf, compbuf,
    table, split, dends, dpar, dst, dmult, dlim, hot, acc,
    mout, dout, lout, sqbuf, rowbuf,
    local, send, recv, ends_recv, ends_recv2,
):
    grp, me = lax.axis_index("ctg"), lax.axis_index("br")
    core = lax.rem(grp, 2)
    shares = pown.shape[0]
    line = lax.rem(grp, groups // (shares // 2)) - core
    part = 2 * (grp // (groups // (shares // 2))) + core
    sibling = grp + 1 - 2 * core
    scen, _, nb = delta_any.shape
    rows = from_any.shape[0]
    btiles = nb // LANES
    tiles = table.shape[1]
    f32, bf16 = jnp.float32, jnp.bfloat16
    piece_len = vm_any.shape[1]

    def fetch(i, src, dst):
        copy = pltpu.make_async_copy(src, dst, local.at[i])
        copy.start()
        return copy

    ends_in = [fetch(2, from_any, ebuf.at[me, 0]), fetch(3, to_any, ebuf.at[me, 1])]
    base_in = [fetch(0, vm_any, vm1), fetch(1, va_any, va1)]
    status_in = [fetch(4, status_any, st8), fetch(5, slack_any, sl8), fetch(6, zdual_any, zd8), fetch(7, rating_any, rate)]
    params_in = [fetch(8, g_any, pstg.at[0]), fetch(9, b_any, pstg.at[1]), fetch(10, h_any, pstg.at[2])]
    bus_in = [fetch(11, delta_any, dstg), fetch(12, mult_any, mstg)]
    late_in = [fetch(13, net_any, nstg), fetch(14, ang_any, ang8)]

    barrier = pltpu.get_barrier_semaphore()

    def greet_near(i, carry):
        pl.semaphore_signal(barrier, inc=1, device_id=(grp, lax.rem(me + i, ranks)), device_id_type=MESH)
        return carry

    def greet_far(i, carry):
        pl.semaphore_signal(barrier, inc=1, device_id=(lax.rem(grp + i, groups), me), device_id_type=MESH)
        return carry

    lax.fori_loop(1, ranks, greet_near, 0)
    lax.fori_loop(1, groups, greet_far, 0)

    for copy in base_in + status_in:
        copy.wait()

    lane = lax.broadcasted_iota(jnp.int32, (SUB, LANES), 1)
    pad = jnp.zeros((1, LANES - piece_len), f32)
    piece = jnp.concatenate(
        [jnp.concatenate([vm1[...], pad], axis=1), jnp.concatenate([va1[...], pad], axis=1), jnp.zeros((SUB - 2, LANES), f32)],
        axis=0,
    )
    shift = lax.rem(grp * (ranks * piece_len) + me * piece_len, LANES)
    piece = pltpu.roll(piece, shift, 1)
    zbuf[me] = piece[0:2, :]

    for r in range(rows):
        cols = slice(r * LANES, (r + 1) * LANES)
        ststg[:, r, :] = st8[:, cols]
        wstg[:, r, :] = sl8[:, cols]
    squared = rate[...] * rate[...]
    for s in range(scen):
        wstg[s] = wstg[s] - squared
    comp = st8[...].astype(f32) * (zd8[...] * sl8[...] - 0.01)
    cstg[:, 0, :] = jnp.broadcast_to(jnp.sum(comp * comp, axis=1, keepdims=True), (scen, LANES))

    for copy in ends_in + params_in + bus_in + late_in:
        copy.wait()
    share = pown.shape[1]
    for j in range(3 * rows):
        q, r = j // rows, j % rows
        pown[j // share, j % share : j % share + 1, :] = pstg[q, r : r + 1, :]
    for j in range(3 * rows, pown.shape[0] * share):
        pown[j // share, j % share : j % share + 1, :] = jnp.zeros((1, LANES), f32)
    for k in range(btiles):
        astg[:, k, :] = ang8[:, k * LANES : (k + 1) * LANES]

    pl.semaphore_wait(barrier, ranks - 1 + groups - 1)

    def near(kind, step, src, dst):
        pltpu.make_async_remote_copy(
            src_ref=src, dst_ref=dst, send_sem=send.at[kind], recv_sem=recv.at[kind],
            device_id=(grp, lax.rem(me + step, ranks)), device_id_type=MESH,
        ).start()

    def far(kind, step, src, dst):
        pltpu.make_async_remote_copy(
            src_ref=src, dst_ref=dst, send_sem=send.at[kind], recv_sem=recv.at[kind],
            device_id=(lax.rem(grp + step, groups), me), device_id_type=MESH,
        ).start()

    def whole(kind, ref, n):
        part = ref.at[pl.ds(0, n)]
        return pltpu.make_async_remote_copy(
            src_ref=part, dst_ref=part, send_sem=send.at[kind], recv_sem=recv.at[kind],
            device_id=(sibling, me), device_id_type=MESH,
        )

    def to_near(kind, src_of, dst):
        def go(step, carry):
            near(kind, step, src_of(lax.rem(me + step, ranks)), dst)
            return carry
        lax.fori_loop(1, ranks, go, 0)

    def to_far(kind, src, dst):
        def go(step, carry):
            far(kind, step, src, dst)
            return carry
        lax.fori_loop(1, groups, go, 0)

    to_near(PIECE, lambda p: zbuf.at[me], zbuf.at[me])

    @pl.when(core == 1)
    def _():
        def send_ends(step, carry):
            pltpu.make_async_remote_copy(
                src_ref=ebuf.at[me], dst_ref=ebuf.at[me], send_sem=send.at[ENDS], recv_sem=ends_recv.at[ranks - step],
                device_id=(grp, lax.rem(me + step, ranks)), device_id_type=MESH,
            ).start()
            return carry

        lax.fori_loop(1, ranks, send_ends, 0)

    to_near(PARAMS, lambda p: pown.at[part], pz.at[me])
    to_near(MULT, lambda p: mstg.at[p], mbuf.at[me])
    to_near(DELTA, lambda p: dstg.at[p], dbuf.at[me])
    to_near(STATUS, lambda p: ststg.at[p], stbuf.at[me])
    to_near(COMP, lambda p: cstg.at[p], compbuf.at[me])
    to_near(NET, lambda p: nstg.at[p], nbuf.at[me])
    to_near(WORK, lambda p: wstg.at[p], wbuf.at[me])
    to_near(ANG, lambda p: astg.at[p], abuf.at[me])

    pz[me] = pown[part]
    stbuf[me] = ststg[me]
    dbuf[me] = dstg[me]
    mbuf[me] = mstg[me]
    nbuf[me] = nstg[me]
    wbuf[me] = wstg[me]
    abuf[me] = astg[me]
    compbuf[me] = cstg[me]
    acc[...] = jnp.zeros_like(acc)

    source = [lax.rem(me + j, ranks) for j in range(ranks)]
    chunks = dends.shape[1] // SUB
    high = acc.shape[0] // 6
    column0 = lax.broadcasted_iota(jnp.int32, (LANES, LANES), 1)
    labels = [(column0 + k * LANES).astype(bf16) for k in range(SPAN // LANES)]
    steps = lax.broadcasted_iota(jnp.int32, (high, LANES), 0).astype(bf16)

    def at_rows(i):
        return pl.ds(pl.multiple_of(i * SUB, SUB), SUB)

    def spread(x, n):
        return jnp.concatenate([jnp.broadcast_to(x, (2 * SUB, LANES)).astype(bf16)] * (n // (2 * SUB)), axis=0)

    def make_hot(step):
        origin = lax.rem(me + step, ranks)
        for end in range(2):
            low = ebuf[origin, end] & (SPAN - 1)
            for r in range(rows):
                spots = spread(low[r : r + 1, :], LANES).T
                place = pl.ds(pl.multiple_of((step * rows + r) * LANES, LANES), LANES)
                for k, label in enumerate(labels):
                    hot[end, k, place, :] = jnp.where(spots == label, bf16(1), bf16(0))

    def ends_copy(sems, origin, step):
        return pltpu.make_async_remote_copy(
            src_ref=ebuf.at[origin], dst_ref=ebuf.at[origin], send_sem=send.at[ENDS2], recv_sem=sems.at[step],
            device_id=(sibling, me), device_id_type=MESH,
        )

    make_hot(0)

    def arrive(t, carry):
        step = jnp.where(lax.rem(t, 2) == 1, (t + 1) // 2, ranks - t // 2)
        origin = lax.rem(me + step, ranks)

        @pl.when(core == 1)
        def _():
            ends_copy(ends_recv, origin, step).wait_recv()
            ends_copy(ends_recv2, origin, step).start()

        @pl.when(core == 0)
        def _():
            ends_copy(ends_recv2, origin, step).wait_recv()

        make_hot(step)
        return carry

    early = 3
    lax.fori_loop(1, early, arrive, 0)

    whole(PIECE, zbuf, ranks - 1).wait_recv()
    window = (LANES // 2) * core
    for m in range(3):
        off = m * LANES + lane[0:2, :] - window
        found = jnp.zeros((2, LANES), f32)
        for b in range(ranks):
            inside = (off >= b * piece_len) & (off < (b + 1) * piece_len)
            found = jnp.where(inside, zbuf[b], found)
        cbuf[grp, m : m + 1, :] = found[0:1, :]
        cbuf[grp, 3 + m : 4 + m, :] = found[1:2, :]
    cbuf[grp, 6:8, :] = jnp.zeros((2, LANES), f32)
    to_far(BASE, cbuf.at[grp], cbuf.at[grp])

    lax.fori_loop(early, ranks, arrive, 0)
    for end in range(2):
        for j in range(ranks):
            dends[end, j * rows : (j + 1) * rows, :] = ebuf[source[j], end]

    whole(PARAMS, pz, ranks - 1).wait_recv()
    pall[part] = pz[...]

    def share_params(d, carry):
        other = lax.rem(part + d, shares)
        pltpu.make_async_remote_copy(
            src_ref=pz, dst_ref=pall.at[part], send_sem=send.at[PARAMS2], recv_sem=recv.at[PARAMS2],
            device_id=((other // 2) * (groups // (shares // 2)) + line + lax.rem(other, 2), me), device_id_type=MESH,
        ).start()
        return carry

    lax.fori_loop(1, shares, share_params, 0)

    whole(MULT, mbuf, ranks - 1).wait_recv()
    for z in range(ranks):
        for q in range(2):
            for k in range(btiles):
                at = z * btiles + k
                table[2 + q, at : at + 1, :] = mbuf[z, q : q + 1, k * LANES : (k + 1) * LANES]

    for q in range(2):
        x = table[2 + q]
        top = x.astype(bf16)
        split[q * tiles : (q + 1) * tiles, 0:LANES] = top
        split[q * tiles : (q + 1) * tiles, LANES : 2 * LANES] = (x - top.astype(f32)).astype(bf16)

    def pick_end(i, end, first):
        spot = dends[end, at_rows(i), :]
        low, tile = spot & (LANES - 1), spot >> 7
        found = [jnp.zeros((SUB, LANES), f32) for _ in range(2)]
        for k in range(tiles):
            here = tile == k
            for q in range(2):
                row = jnp.broadcast_to(table[first + q, k : k + 1, :], (SUB, LANES))
                got = jnp.take_along_axis(row, low, axis=1, mode="promise_in_bounds")
                found[q] = jnp.where(here, got, found[q])
        return found

    def pick(i, first):
        return tuple(pick_end(i, 0, first) + pick_end(i, 1, first))

    lane_row = lax.broadcasted_iota(jnp.int32, (LANES, LANES), 0).astype(bf16)
    sublane = lax.broadcasted_iota(jnp.int32, (SUB, LANES), 0)

    def pick_by_matmul(i, end):
        spot = dends[end, at_rows(i), :]
        low, tile = spot & (LANES - 1), spot >> 7
        found = [[], []]
        for r in range(0, SUB, 2):
            ones = jnp.concatenate(
                [jnp.where(spread(low[k : k + 1, :], LANES) == lane_row, bf16(1), bf16(0)) for k in (r, r + 1)], axis=1
            )
            got = jnp.dot(split[...], jnp.concatenate([ones, ones], axis=0), preferred_element_type=f32)
            for k in range(2):
                at = jnp.broadcast_to(tile[r + k : r + k + 1, :], (SUB, LANES)) - sublane
                sums = [jnp.zeros((SUB, LANES), f32) for _ in range(2)]
                for j in range(tiles // SUB):
                    here = at == j * SUB
                    for q in range(2):
                        top = q * tiles + j * SUB
                        sums[q] = jnp.where(here, got[top : top + SUB, k * LANES : (k + 1) * LANES], sums[q])
                for q in range(2):
                    found[q].append(jnp.sum(sums[q], axis=0, keepdims=True))
        return [jnp.concatenate(x, axis=0) for x in found]

    def keep(i):
        for k, x in enumerate(pick_end(i, 0, 2) + pick_by_matmul(i, 1)):
            dmult[k, at_rows(i), :] = x

    unit = 4

    def keep_unit(j, carry):
        for k in range(unit):
            keep(unit * j + k)
        return carry

    lax.fori_loop(0, chunks // unit, keep_unit, 0)
    for i in range(chunks // unit * unit, chunks):
        keep(i)

    whole(DELTA, dbuf, ranks - 1).wait_recv()
    whole(BASE, cbuf, groups - 1).wait_recv()

    for r in range(groups // 2):
        for q in range(2):
            def one(c, m):
                return cbuf[2 * r + c, 3 * q + m : 3 * q + m + 1, :]
            five = (one(0, 0), one(0, 1), one(0, 2) + one(1, 0), one(1, 1), one(1, 2))
            for m in range(5):
                at = 5 * r + m
                z, k = at // btiles, at % btiles
                table[q, at : at + 1, :] = five[m] + dbuf[z, q : q + 1, k * LANES : (k + 1) * LANES]

    def scatter(i, picked):
        vf, af, vt, at = picked
        where_ = at_rows(i)
        mpf, mqf, mpt, mqt = (dmult[k, where_, :] for k in range(4))
        sn, cs = sin_cos(af - at)
        g, b, h = dpar[0, where_, :], dpar[1, where_, :], dpar[2, where_, :]
        live = dst[where_, :].astype(f32)
        u = vf * vt
        gc_bs, gc_mbs = g * cs + b * sn, g * cs - b * sn
        gs_bc, gs_mbc = g * sn + b * cs, g * sn - b * cs
        bh = -(b + h)
        pf = live * (g * vf * vf - u * gc_bs)
        qf = live * (bh * vf * vf - u * gs_mbc)
        pt = live * (g * vt * vt - u * gc_mbs)
        qt = live * (bh * vt * vt + u * gs_bc)
        fd = live * u * (mpf * gs_mbc - mqf * gc_bs + mpt * gs_bc + mqt * gc_mbs)
        dlim[where_, :] = pf * pf + qf * qf
        total = None
        for end, terms in ((0, (pf, qf, fd)), (1, (pt, qt, -fd))):
            parts = []
            for value in terms:
                head = value.astype(bf16).astype(f32)
                parts += [head, value - head]
            tile = dends[end, where_, :] >> 8
            lefts = []
            for r in range(SUB):
                row = slice(r, r + 1)
                mask = spread(tile[row, :], high) == steps
                lefts.append(jnp.concatenate(
                    [jnp.where(mask, spread(x[row, :], high), bf16(0)) for x in parts], axis=0
                ))
            spots = pl.ds(pl.multiple_of(i * (SUB * LANES), SUB * LANES), SUB * LANES)
            right = jnp.concatenate([hot[end, k, spots, :] for k in range(SPAN // LANES)], axis=1)
            dot = lax.dot_general(
                jnp.concatenate(lefts, axis=1), right, (((1,), (0,)), ((), ())), preferred_element_type=f32
            )
            total = dot if total is None else total + dot
        return total

    def two(i):
        return pick(i, 0) + pick(i + 1, 0)

    def scatter_two(i, picked):
        acc[...] += scatter(i, picked[:4]) + scatter(i + 1, picked[4:])

    def advance(j, picked):
        following = two(2 * j + 1)
        scatter_two(2 * j - 1, picked)
        return following

    first = pick(0, 0)

    whole(STATUS, stbuf, ranks - 1).wait_recv()
    for j in range(ranks):
        dst[j * rows : (j + 1) * rows, :] = stbuf[source[j]]

    whole(PARAMS2, pall, shares - 1).wait_recv()
    for j in range(ranks):
        for k in range(3 * rows):
            q, r = k // rows, j * rows + k % rows
            dpar[q, r : r + 1, :] = pall[k // share, source[j], k % share : k % share + 1, :]

    following = two(1)
    acc[...] += scatter(0, first)
    scatter_two(chunks - 2, lax.fori_loop(1, chunks // 2, advance, following))

    whole(NET, nbuf, ranks - 1).wait_recv()
    whole(WORK, wbuf, ranks - 1).wait_recv()
    whole(ANG, abuf, ranks - 1).wait_recv()
    whole(COMP, compbuf, ranks - 1).wait_recv()

    per = nb // SPAN
    mis_sq = jnp.zeros((1, SPAN), f32)
    dual_sq = jnp.zeros((1, LANES), f32)
    for z in range(ranks):
        for j in range(per):
            t = z * per + j
            cols = slice(j * SPAN, (j + 1) * SPAN)
            for q in range(3):
                top, bottom = (2 * q) * high + t, (2 * q + 1) * high + t
                row = acc[top : top + 1, :] + acc[bottom : bottom + 1, :]
                if q < 2:
                    row = row - nbuf[z, q : q + 1, cols]
                    mout[z, q : q + 1, cols] = row
                    mis_sq = mis_sq + row * row
                else:
                    for half in range(2):
                        k = 2 * j + half
                        one = row[:, half * LANES : (half + 1) * LANES] + abuf[z, k : k + 1, :]
                        dout[z, k : k + 1, :] = one
                        dual_sq = dual_sq + one * one
    lim_sq = jnp.zeros((rows, LANES), f32)
    for j in range(ranks):
        z = source[j]
        lim = stbuf[z].astype(f32) * (dlim[j * rows : (j + 1) * rows, :] + wbuf[z])
        lout[z] = lim
        lim_sq = lim_sq + lim * lim
    comp_sq = jnp.zeros((1, LANES), f32)
    for z in range(ranks):
        comp_sq = comp_sq + compbuf[z]

    def total_of(x):
        return jnp.sum(jnp.sum(x, axis=0, keepdims=True), axis=1, keepdims=True)

    lane1 = lane[0:1, :]
    squares = jnp.where(
        lane1 == 0, total_of(mis_sq),
        jnp.where(lane1 == 1, total_of(dual_sq), jnp.where(lane1 == 2, total_of(lim_sq), jnp.where(lane1 == 3, comp_sq, 0.0))),
    )
    sqbuf[me] = squares
    to_near(SQ, lambda p: sqbuf.at[me], sqbuf.at[me])
    to_near(MIS, lambda p: mout.at[p], min_.at[me])
    to_near(DUAL, lambda p: dout.at[p], din.at[me])
    to_near(LIM, lambda p: lout.at[p], lin.at[me])
    min_[me] = mout[me]
    din[me] = dout[me]
    lin[me] = lout[me]

    whole(SQ, sqbuf, ranks - 1).wait_recv()
    column = jnp.zeros((1, LANES), f32)
    for z in range(ranks):
        one = sqbuf[z]
        column = column + one
        norm_out[z : z + 1, :] = jnp.sqrt(one)
    rowbuf[grp] = column
    to_far(TOTAL, rowbuf.at[grp], rowbuf.at[grp])

    whole(MIS, min_, ranks - 1).wait_recv()
    whole(DUAL, din, ranks - 1).wait_recv()
    whole(LIM, lin, ranks - 1).wait_recv()

    @pl.when(core == 1)
    def _():
        whole(ENDS, ebuf, ranks - 1).wait_send()
        whole(ENDS2, ebuf, ranks - 1).wait_send()

    whole(PARAMS, pown, ranks - 1).wait_send()
    whole(PARAMS2, pall, shares - 1).wait_send()
    for kind, ref in (
        (PIECE, zbuf), (STATUS, ststg), (DELTA, dstg), (MULT, mstg), (COMP, cstg), (NET, nstg), (WORK, wstg),
        (ANG, astg), (SQ, sqbuf), (MIS, mout), (DUAL, dout), (LIM, lout),
    ):
        whole(kind, ref, ranks - 1).wait_send()
    whole(BASE, cbuf, groups - 1).wait_send()
    whole(TOTAL, rowbuf, groups - 1).wait_send()

    whole(TOTAL, rowbuf, groups - 1).wait_recv()
    everything = jnp.zeros((1, LANES), f32)
    for i in range(groups):
        everything = everything + rowbuf[i]
    tot_out[...] = jnp.sqrt(everything[:, 0:4] / (scen * groups))


def write_out(min_, din, lin, norms, tot, mis_any, dual_any, lim_any, norm_any, tot_any, dual, lim, turned, sems):
    copies = [
        pltpu.make_async_copy(src, dst, sems.at[i])
        for i, (src, dst) in enumerate((
            (min_, mis_any), (tot, tot_any), (dual, dual_any), (lim, lim_any), (turned, norm_any),
        ))
    ]
    copies[0].start()
    copies[1].start()
    for k in range(din.shape[1]):
        dual[:, k * LANES : (k + 1) * LANES] = din[:, k, :]
    copies[2].start()
    for r in range(lin.shape[1]):
        lim[:, r * LANES : (r + 1) * LANES] = lin[:, r, :]
    copies[3].start()
    turned[...] = norms[...].T[0:4, :]
    copies[4].start()
    for copy in copies:
        copy.wait()


def per_device(
    base_vm, base_va, delta_state, multipliers, net_inj, ang_grad, from_bus, to_bus,
    status, conduct, suscept, charging, rating, slack, zdual,
):
    groups, ranks = lax.axis_size("ctg"), lax.axis_size("br")
    scen, _, nb = delta_state.shape
    nl = from_bus.shape[0]
    rows, btiles = nl // LANES, nb // LANES
    buses = nb * ranks
    tiles = buses // LANES
    high = -(-(buses // SPAN) // 16) * 16
    block = base_vm.shape[0]
    shares = 8
    share = -(-3 * rows // shares)
    f32, i32 = jnp.float32, jnp.int32
    vmem = pl.BlockSpec(memory_space=pltpu.VMEM)
    hbm = pl.BlockSpec(memory_space=pltpu.HBM)
    V = pltpu.VMEM
    outs = pl.pallas_call(
        functools.partial(body, groups, ranks),
        out_shape=(
            jax.ShapeDtypeStruct((ranks, 2, nb), f32),
            jax.ShapeDtypeStruct((ranks, btiles, LANES), f32),
            jax.ShapeDtypeStruct((ranks, rows, LANES), f32),
            jax.ShapeDtypeStruct((scen, LANES), f32),
            jax.ShapeDtypeStruct((1, 4), f32),
        ),
        in_specs=[hbm] * 15,
        out_specs=(vmem,) * 5,
        scratch_shapes=[
            V((1, block), f32), V((1, block), f32),
            V((scen, 2, nb), f32), V((scen, 2, nb), f32), V((scen, 2, nb), f32),
            V((scen, nb), f32), V((scen, nl), i32), V((scen, nl), f32), V((scen, nl), f32), V((rows, LANES), f32),
            V((scen, rows, LANES), i32), V((scen, rows, LANES), f32), V((scen, btiles, LANES), f32), V((scen, 1, LANES), f32),
            V((3, rows, LANES), f32), V((shares, share, LANES), f32), V((ranks, share, LANES), f32),
            V((shares, ranks, share, LANES), f32), V((ranks, 2, rows, LANES), i32),
            V((ranks, rows, LANES), i32),
            V((ranks, 2, nb), f32), V((ranks, 2, nb), f32), V((ranks, 2, LANES), f32), V((groups, SUB, LANES), f32),
            V((ranks, 2, nb), f32), V((ranks, rows, LANES), f32), V((ranks, btiles, LANES), f32), V((ranks, 1, LANES), f32),
            V((4, tiles, LANES), f32), V((2 * tiles, 2 * LANES), jnp.bfloat16), V((2, ranks * rows, LANES), i32), V((3, ranks * rows, LANES), f32),
            V((ranks * rows, LANES), i32), V((4, ranks * rows, LANES), f32), V((ranks * rows, LANES), f32),
            V((2, SPAN // LANES, ranks * nl, LANES), jnp.bfloat16), V((6 * high, SPAN), f32),
            V((ranks, 2, nb), f32), V((ranks, btiles, LANES), f32), V((ranks, rows, LANES), f32),
            V((ranks, 1, LANES), f32), V((groups, 1, LANES), f32),
            pltpu.SemaphoreType.DMA((15,)),
            pltpu.SemaphoreType.DMA((KINDS,)),
            pltpu.SemaphoreType.DMA((KINDS,)),
            pltpu.SemaphoreType.DMA((ranks,)),
            pltpu.SemaphoreType.DMA((ranks,)),
        ],
        compiler_params=pltpu.CompilerParams(
            collective_id=0, has_side_effects=True, vmem_limit_bytes=40 << 20
        ),
    )(*(pltpu.with_memory_space_constraint(x, pltpu.HBM) for x in (
        base_vm[None, :], base_va[None, :], delta_state, multipliers, net_inj, ang_grad,
        *(x.reshape(rows, LANES) for x in (from_bus, to_bus, conduct, suscept, charging, rating)),
        status, slack, zdual,
    )))
    mis, dual, lim, norms, tot = pl.pallas_call(
        write_out,
        out_shape=(
            jax.ShapeDtypeStruct((scen, 2, nb), f32),
            jax.ShapeDtypeStruct((scen, nb), f32),
            jax.ShapeDtypeStruct((scen, nl), f32),
            jax.ShapeDtypeStruct((4, scen), f32),
            jax.ShapeDtypeStruct((1, 4), f32),
        ),
        in_specs=[vmem] * 5,
        out_specs=(pl.BlockSpec(memory_space=pl.ANY),) * 5,
        scratch_shapes=[
            V((scen, nb), f32), V((scen, nl), f32), V((4, scen), f32), pltpu.SemaphoreType.DMA((5,)),
        ],
        compiler_params=pltpu.CompilerParams(vmem_limit_bytes=8 << 20),
    )(*outs)
    return (mis, dual, lim, norms.T, tot[0])


def solution(mesh):
    placed = (
        P(("ctg", "br")), P(("ctg", "br")),
        P("ctg", None, "br"), P("ctg", None, "br"), P("ctg", None, "br"), P("ctg", "br"),
        P("br"), P("br"), P("ctg", "br"), P("br"), P("br"), P("br"), P("br"),
        P("ctg", "br"), P("ctg", "br"),
    )
    return jax.shard_map(
        per_device,
        mesh=mesh,
        in_specs=placed,
        out_specs=(P("ctg", None, "br"), P("ctg", "br"), P("ctg", "br"), P("ctg", None), P()),
        check_vma=False,
    )
```

```python
import functools

import jax
import jax.numpy as jnp
from jax import lax
from jax.experimental import pallas as pl
from jax.experimental.pallas import tpu as pltpu
from jax.sharding import PartitionSpec as P

LANES = 128
SUB = 8
SPAN = 256
MESH = pl.DeviceIdType.MESH

ENDS, PARAMS, STATUS, MULT, DELTA, PIECE, BASE, NET, WORK, ANG, COMP, ENDS2, PARAMS2, SQ, MIS, DUAL, LIM, TOTAL = range(18)
KINDS = 18


def sin_cos(x):
    y = x * x
    sin_c = (1 / 6227020800, -1 / 39916800, 1 / 362880, -1 / 5040, 1 / 120, -1 / 6)
    cos_c = (-1 / 87178291200, 1 / 479001600, -1 / 3628800, 1 / 40320, -1 / 720, 1 / 24, -0.5)
    s = jnp.full_like(y, sin_c[0])
    for c in sin_c[1:]:
        s = s * y + c
    k = jnp.full_like(y, cos_c[0])
    for c in cos_c[1:]:
        k = k * y + c
    return x + x * y * s, 1.0 + y * k


def body(
    groups, ranks,
    vm_any, va_any, delta_any, mult_any, net_any, ang_any, from_any, to_any,
    g_any, b_any, h_any, rating_any, status_any, slack_any, zdual_any,
    min_, din, lin, norm_out, tot_out,
    vm1, va1, dstg, mstg, nstg, ang8, st8, sl8, zd8, rate,
    ststg, wstg, astg, cstg,
    pstg, pown, pz, pall, ebuf, stbuf, mbuf, dbuf, zbuf, cbuf, nbuf, wbuf, abuf, compbuf,
    table, split, dends, dpar, dst, dmult, dlim, hot, acc,
    mout, dout, lout, sqbuf, rowbuf,
    send, recv, ends_recv, ends_recv2,
):
    grp, me = lax.axis_index("ctg"), lax.axis_index("br")
    core = lax.rem(grp, 2)
    shares = pown.shape[0]
    line = lax.rem(grp, groups // (shares // 2)) - core
    part = 2 * (grp // (groups // (shares // 2))) + core
    sibling = grp + 1 - 2 * core
    scen, _, nb = delta_any.shape
    rows = from_any.shape[0]
    btiles = nb // LANES
    tiles = table.shape[1]
    f32, bf16 = jnp.float32, jnp.bfloat16
    piece_len = vm_any.shape[1]

    def fetch(i, src, dst):
        copy = pltpu.make_async_copy(src, dst, send.at[i])
        copy.start()
        return copy

    ends_in = [fetch(2, from_any, ebuf.at[me, 0]), fetch(3, to_any, ebuf.at[me, 1])]
    base_in = [fetch(0, vm_any, vm1), fetch(1, va_any, va1)]
    status_in = [fetch(4, status_any, st8), fetch(5, slack_any, sl8), fetch(6, zdual_any, zd8), fetch(7, rating_any, rate)]
    params_in = [fetch(8, g_any, pstg.at[0]), fetch(9, b_any, pstg.at[1]), fetch(10, h_any, pstg.at[2])]
    bus_in = [fetch(11, delta_any, dstg), fetch(12, mult_any, mstg)]
    late_in = [fetch(13, net_any, nstg), fetch(14, ang_any, ang8)]

    barrier = pltpu.get_barrier_semaphore()

    def outward(n):
        return [n // 2 + ((i + 1) // 2 if i % 2 else -(i // 2)) for i in range(n - 1)]

    near_steps = outward(ranks)
    near_peers = {step: lax.rem(me + step, ranks) for step in near_steps}

    for step in near_steps:
        pl.semaphore_signal(barrier, inc=1, device_id=(grp, near_peers[step]), device_id_type=MESH)
    for step in outward(groups):
        pl.semaphore_signal(barrier, inc=1, device_id=(lax.rem(grp + step, groups), me), device_id_type=MESH)

    for copy in base_in + status_in:
        copy.wait()

    lane = lax.broadcasted_iota(jnp.int32, (SUB, LANES), 1)
    pad = jnp.zeros((1, LANES - piece_len), f32)
    piece = jnp.concatenate(
        [jnp.concatenate([vm1[...], pad], axis=1), jnp.concatenate([va1[...], pad], axis=1), jnp.zeros((SUB - 2, LANES), f32)],
        axis=0,
    )
    shift = lax.rem(grp * (ranks * piece_len) + me * piece_len, LANES)
    piece = pltpu.roll(piece, shift, 1)
    zbuf[me] = piece[0:2, :]

    for r in range(rows):
        cols = slice(r * LANES, (r + 1) * LANES)
        ststg[:, r, :] = st8[:, cols]
        wstg[:, r, :] = sl8[:, cols]
    squared = rate[...] * rate[...]
    for s in range(scen):
        wstg[s] = wstg[s] - squared
    comp = st8[...].astype(f32) * (zd8[...] * sl8[...] - 0.01)
    cstg[:, 0, :] = jnp.broadcast_to(jnp.sum(comp * comp, axis=1, keepdims=True), (scen, LANES))

    for copy in ends_in + params_in + bus_in + late_in:
        copy.wait()
    share = pown.shape[1]
    for j in range(3 * rows):
        q, r = j // rows, j % rows
        pown[j // share, j % share : j % share + 1, :] = pstg[q, r : r + 1, :]
    for j in range(3 * rows, pown.shape[0] * share):
        pown[j // share, j % share : j % share + 1, :] = jnp.zeros((1, LANES), f32)
    for k in range(btiles):
        astg[:, k, :] = ang8[:, k * LANES : (k + 1) * LANES]

    pl.semaphore_wait(barrier, ranks - 1 + groups - 1)

    def near(kind, step, src, dst):
        pltpu.make_async_remote_copy(
            src_ref=src, dst_ref=dst, send_sem=send.at[kind], recv_sem=recv.at[kind],
            device_id=(grp, near_peers[step]), device_id_type=MESH,
        ).start()

    def far(kind, step, src, dst):
        pltpu.make_async_remote_copy(
            src_ref=src, dst_ref=dst, send_sem=send.at[kind], recv_sem=recv.at[kind],
            device_id=(lax.rem(grp + step, groups), me), device_id_type=MESH,
        ).start()

    def whole(kind, ref, n):
        part = ref.at[pl.ds(0, n)]
        return pltpu.make_async_remote_copy(
            src_ref=part, dst_ref=part, send_sem=send.at[kind], recv_sem=recv.at[kind],
            device_id=(sibling, me), device_id_type=MESH,
        )

    def to_near(kind, src_of, dst):
        for step in near_steps:
            near(kind, step, src_of(near_peers[step]), dst)

    def to_far(kind, src, dst):
        for step in outward(groups):
            far(kind, step, src, dst)

    to_near(PIECE, lambda p: zbuf.at[me], zbuf.at[me])

    @pl.when(core == 1)
    def _():
        def send_ends(step, carry):
            pltpu.make_async_remote_copy(
                src_ref=ebuf.at[me], dst_ref=ebuf.at[me], send_sem=send.at[ENDS], recv_sem=ends_recv.at[ranks - step],
                device_id=(grp, lax.rem(me + step, ranks)), device_id_type=MESH,
            ).start()
            return carry

        lax.fori_loop(1, ranks, send_ends, 0)

    to_near(PARAMS, lambda p: pown.at[part], pz.at[me])
    to_near(MULT, lambda p: mstg.at[p], mbuf.at[me])
    to_near(DELTA, lambda p: dstg.at[p], dbuf.at[me])
    to_near(STATUS, lambda p: ststg.at[p], stbuf.at[me])

    pz[me] = pown[part]
    stbuf[me] = ststg[me]
    dbuf[me] = dstg[me]
    mbuf[me] = mstg[me]
    nbuf[me] = nstg[me]
    wbuf[me] = wstg[me]
    abuf[me] = astg[me]
    compbuf[me] = cstg[me]
    acc[...] = jnp.zeros_like(acc)

    source = [lax.rem(me + j, ranks) for j in range(ranks)]
    chunks = dends.shape[1] // SUB
    high = acc.shape[0] // 6
    column0 = lax.broadcasted_iota(jnp.int32, (LANES, LANES), 1)
    labels = [(column0 + k * LANES).astype(bf16) for k in range(SPAN // LANES)]
    steps = lax.broadcasted_iota(jnp.int32, (high, LANES), 0).astype(bf16)

    def at_rows(i):
        return pl.ds(pl.multiple_of(i * SUB, SUB), SUB)

    def spread(x, n):
        return jnp.concatenate([jnp.broadcast_to(x, (2 * SUB, LANES)).astype(bf16)] * (n // (2 * SUB)), axis=0)

    def make_hot(step):
        origin = lax.rem(me + step, ranks)
        for end in range(2):
            low = ebuf[origin, end] & (SPAN - 1)
            for r in range(rows):
                spots = spread(low[r : r + 1, :], LANES).T
                place = pl.ds(pl.multiple_of((step * rows + r) * LANES, LANES), LANES)
                for k, label in enumerate(labels):
                    hot[end, k, place, :] = jnp.where(spots == label, bf16(1), bf16(0))

    def ends_copy(sems, origin, step):
        return pltpu.make_async_remote_copy(
            src_ref=ebuf.at[origin], dst_ref=ebuf.at[origin], send_sem=send.at[ENDS2], recv_sem=sems.at[step],
            device_id=(sibling, me), device_id_type=MESH,
        )

    make_hot(0)

    def arrive(t, carry):
        step = jnp.where(lax.rem(t, 2) == 1, (t + 1) // 2, ranks - t // 2)
        origin = lax.rem(me + step, ranks)

        @pl.when(core == 1)
        def _():
            ends_copy(ends_recv, origin, step).wait_recv()
            ends_copy(ends_recv2, origin, step).start()

        @pl.when(core == 0)
        def _():
            ends_copy(ends_recv2, origin, step).wait_recv()

        make_hot(step)
        return carry

    early = 3
    lax.fori_loop(1, early, arrive, 0)

    whole(PIECE, zbuf, ranks - 1).wait_recv()
    window = (LANES // 2) * core
    for m in range(3):
        off = m * LANES + lane[0:2, :] - window
        found = jnp.zeros((2, LANES), f32)
        for b in range(ranks):
            inside = (off >= b * piece_len) & (off < (b + 1) * piece_len)
            found = jnp.where(inside, zbuf[b], found)
        cbuf[grp, m : m + 1, :] = found[0:1, :]
        cbuf[grp, 3 + m : 4 + m, :] = found[1:2, :]
    to_far(BASE, cbuf.at[grp], cbuf.at[grp])

    lax.fori_loop(early, ranks - 2, arrive, 0)

    whole(PARAMS, pz, ranks - 1).wait_recv()
    pall[part] = pz[...]

    def share_params(d, carry):
        other = lax.rem(part + d, shares)
        pltpu.make_async_remote_copy(
            src_ref=pz, dst_ref=pall.at[part], send_sem=send.at[PARAMS2], recv_sem=recv.at[PARAMS2],
            device_id=((other // 2) * (groups // (shares // 2)) + line + lax.rem(other, 2), me), device_id_type=MESH,
        ).start()
        return carry

    lax.fori_loop(1, shares, share_params, 0)

    lax.fori_loop(ranks - 2, ranks, arrive, 0)
    for end in range(2):
        for j in range(ranks):
            dends[end, j * rows : (j + 1) * rows, :] = ebuf[source[j], end]

    whole(MULT, mbuf, ranks - 1).wait_recv()
    for z in range(ranks):
        for q in range(2):
            for k in range(btiles):
                at = z * btiles + k
                table[2 + q, at : at + 1, :] = mbuf[z, q : q + 1, k * LANES : (k + 1) * LANES]

    for q in range(2):
        x = table[2 + q]
        top = x.astype(bf16)
        split[q * tiles : (q + 1) * tiles, 0:LANES] = top
        split[q * tiles : (q + 1) * tiles, LANES : 2 * LANES] = (x - top.astype(f32)).astype(bf16)

    def pick_end(i, end, first):
        spot = dends[end, at_rows(i), :]
        low, tile = spot & (LANES - 1), spot >> 7
        found = [jnp.zeros((SUB, LANES), f32) for _ in range(2)]
        for k in range(tiles):
            here = tile == k
            for q in range(2):
                row = jnp.broadcast_to(table[first + q, k : k + 1, :], (SUB, LANES))
                got = jnp.take_along_axis(row, low, axis=1, mode="promise_in_bounds")
                found[q] = jnp.where(here, got, found[q])
        return found

    def pick(i, first):
        return tuple(pick_end(i, 0, first) + pick_end(i, 1, first))

    to_near(COMP, lambda p: cstg.at[p], compbuf.at[me])
    to_near(NET, lambda p: nstg.at[p], nbuf.at[me])
    to_near(WORK, lambda p: wstg.at[p], wbuf.at[me])
    to_near(ANG, lambda p: astg.at[p], abuf.at[me])

    lane_row = lax.broadcasted_iota(jnp.int32, (LANES, LANES), 0).astype(bf16)
    sublane = lax.broadcasted_iota(jnp.int32, (SUB, LANES), 0)

    def pick_by_matmul(i, end):
        spot = dends[end, at_rows(i), :]
        low, tile = spot & (LANES - 1), spot >> 7
        found = [[], []]
        for r in range(0, SUB, 2):
            ones = jnp.concatenate(
                [jnp.where(spread(low[k : k + 1, :], LANES) == lane_row, bf16(1), bf16(0)) for k in (r, r + 1)], axis=1
            )
            got = jnp.dot(split[...], jnp.concatenate([ones, ones], axis=0), preferred_element_type=f32)
            for k in range(2):
                at = jnp.broadcast_to(tile[r + k : r + k + 1, :], (SUB, LANES)) - sublane
                sums = [jnp.zeros((SUB, LANES), f32) for _ in range(2)]
                for j in range(tiles // SUB):
                    here = at == j * SUB
                    for q in range(2):
                        top = q * tiles + j * SUB
                        sums[q] = jnp.where(here, got[top : top + SUB, k * LANES : (k + 1) * LANES], sums[q])
                for q in range(2):
                    found[q].append(jnp.sum(sums[q], axis=0, keepdims=True))
        return [jnp.concatenate(x, axis=0) for x in found]

    def keep(i):
        for k, x in enumerate(pick_end(i, 0, 2) + pick_by_matmul(i, 1)):
            dmult[k, at_rows(i), :] = x

    unit = 4

    def keep_unit(j, carry):
        for k in range(unit):
            keep(unit * j + k)
        return carry

    lax.fori_loop(0, chunks // unit, keep_unit, 0)
    for i in range(chunks // unit * unit, chunks):
        keep(i)

    whole(DELTA, dbuf, ranks - 1).wait_recv()
    whole(BASE, cbuf, groups - 1).wait_recv()

    for r in range(groups // 2):
        for q in range(2):
            def one(c, m):
                return cbuf[2 * r + c, 3 * q + m : 3 * q + m + 1, :]
            five = (one(0, 0), one(0, 1), one(0, 2) + one(1, 0), one(1, 1), one(1, 2))
            for m in range(5):
                at = 5 * r + m
                z, k = at // btiles, at % btiles
                table[q, at : at + 1, :] = five[m] + dbuf[z, q : q + 1, k * LANES : (k + 1) * LANES]

    def scatter(i, picked):
        vf, af, vt, at = picked
        where_ = at_rows(i)
        mpf, mqf, mpt, mqt = (dmult[k, where_, :] for k in range(4))
        sn, cs = sin_cos(af - at)
        g, b, h = dpar[0, where_, :], dpar[1, where_, :], dpar[2, where_, :]
        live = dst[where_, :].astype(f32)
        u = vf * vt
        gc_bs, gc_mbs = g * cs + b * sn, g * cs - b * sn
        gs_bc, gs_mbc = g * sn + b * cs, g * sn - b * cs
        bh = -(b + h)
        pf = live * (g * vf * vf - u * gc_bs)
        qf = live * (bh * vf * vf - u * gs_mbc)
        pt = live * (g * vt * vt - u * gc_mbs)
        qt = live * (bh * vt * vt + u * gs_bc)
        fd = live * u * (mpf * gs_mbc - mqf * gc_bs + mpt * gs_bc + mqt * gc_mbs)
        dlim[where_, :] = pf * pf + qf * qf
        total = None
        for end, terms in ((0, (pf, qf, fd)), (1, (pt, qt, -fd))):
            parts = []
            for value in terms:
                head = value.astype(bf16).astype(f32)
                parts += [head, value - head]
            tile = dends[end, where_, :] >> 8
            lefts = []
            for r in range(SUB):
                row = slice(r, r + 1)
                mask = spread(tile[row, :], high) == steps
                lefts.append(jnp.concatenate(
                    [jnp.where(mask, spread(x[row, :], high), bf16(0)) for x in parts], axis=0
                ))
            spots = pl.ds(pl.multiple_of(i * (SUB * LANES), SUB * LANES), SUB * LANES)
            right = jnp.concatenate([hot[end, k, spots, :] for k in range(SPAN // LANES)], axis=1)
            dot = lax.dot_general(
                jnp.concatenate(lefts, axis=1), right, (((1,), (0,)), ((), ())), preferred_element_type=f32
            )
            total = dot if total is None else total + dot
        return total

    def two(i):
        return pick(i, 0) + pick(i + 1, 0)

    def scatter_two(i, picked):
        acc[...] += scatter(i, picked[:4]) + scatter(i + 1, picked[4:])

    def advance(j, picked):
        following = two(2 * j + 1)
        scatter_two(2 * j - 1, picked)
        return following

    first = pick(0, 0)

    whole(STATUS, stbuf, ranks - 1).wait_recv()
    for j in range(ranks):
        dst[j * rows : (j + 1) * rows, :] = stbuf[source[j]]

    whole(PARAMS2, pall, shares - 1).wait_recv()
    for j in range(ranks):
        for k in range(3 * rows):
            q, r = k // rows, j * rows + k % rows
            dpar[q, r : r + 1, :] = pall[k // share, source[j], k % share : k % share + 1, :]

    following = two(1)
    acc[...] += scatter(0, first)
    scatter_two(chunks - 2, lax.fori_loop(1, chunks // 2, advance, following))

    whole(NET, nbuf, ranks - 1).wait_recv()
    whole(WORK, wbuf, ranks - 1).wait_recv()
    whole(ANG, abuf, ranks - 1).wait_recv()
    whole(COMP, compbuf, ranks - 1).wait_recv()

    per = nb // SPAN
    mis_sq = jnp.zeros((1, SPAN), f32)
    dual_sq = jnp.zeros((1, LANES), f32)
    for z in range(ranks):
        for j in range(per):
            t = z * per + j
            cols = slice(j * SPAN, (j + 1) * SPAN)
            for q in range(3):
                top, bottom = (2 * q) * high + t, (2 * q + 1) * high + t
                row = acc[top : top + 1, :] + acc[bottom : bottom + 1, :]
                if q < 2:
                    row = row - nbuf[z, q : q + 1, cols]
                    mout[z, q : q + 1, cols] = row
                    mis_sq = mis_sq + row * row
                else:
                    for half in range(2):
                        k = 2 * j + half
                        one = row[:, half * LANES : (half + 1) * LANES] + abuf[z, k : k + 1, :]
                        dout[z, k : k + 1, :] = one
                        dual_sq = dual_sq + one * one
    lim_sq = jnp.zeros((rows, LANES), f32)
    for j in range(ranks):
        z = source[j]
        lim = stbuf[z].astype(f32) * (dlim[j * rows : (j + 1) * rows, :] + wbuf[z])
        lout[z] = lim
        lim_sq = lim_sq + lim * lim
    comp_sq = jnp.zeros((1, LANES), f32)
    for z in range(ranks):
        comp_sq = comp_sq + compbuf[z]

    def total_of(x):
        return jnp.sum(jnp.sum(x, axis=0, keepdims=True), axis=1, keepdims=True)

    lane1 = lane[0:1, :]
    squares = jnp.where(
        lane1 == 0, total_of(mis_sq),
        jnp.where(lane1 == 1, total_of(dual_sq), jnp.where(lane1 == 2, total_of(lim_sq), jnp.where(lane1 == 3, comp_sq, 0.0))),
    )
    sqbuf[me] = squares
    to_near(SQ, lambda p: sqbuf.at[me], sqbuf.at[me])
    to_near(MIS, lambda p: mout.at[p], min_.at[me])
    to_near(DUAL, lambda p: dout.at[p], din.at[me])
    to_near(LIM, lambda p: lout.at[p], lin.at[me])
    min_[me] = mout[me]
    din[me] = dout[me]
    lin[me] = lout[me]

    whole(SQ, sqbuf, ranks - 1).wait_recv()
    column = jnp.zeros((1, LANES), f32)
    for z in range(ranks):
        one = sqbuf[z]
        column = column + one
        norm_out[z : z + 1, :] = jnp.sqrt(one)
    rowbuf[grp] = column
    to_far(TOTAL, rowbuf.at[grp], rowbuf.at[grp])

    whole(MIS, min_, ranks - 1).wait_recv()
    whole(DUAL, din, ranks - 1).wait_recv()
    whole(LIM, lin, ranks - 1).wait_recv()

    @pl.when(core == 1)
    def _():
        whole(ENDS, ebuf, ranks - 1).wait_send()
        whole(ENDS2, ebuf, ranks - 1).wait_send()

    whole(PARAMS, pown, ranks - 1).wait_send()
    whole(PARAMS2, pall, shares - 1).wait_send()
    for kind, ref in (
        (PIECE, zbuf), (STATUS, ststg), (DELTA, dstg), (MULT, mstg), (COMP, cstg), (NET, nstg), (WORK, wstg),
        (ANG, astg), (SQ, sqbuf), (MIS, mout), (DUAL, dout), (LIM, lout),
    ):
        whole(kind, ref, ranks - 1).wait_send()
    whole(BASE, cbuf, groups - 1).wait_send()
    whole(TOTAL, rowbuf, groups - 1).wait_send()

    whole(TOTAL, rowbuf, groups - 1).wait_recv()
    everything = jnp.zeros((1, LANES), f32)
    for i in range(groups):
        everything = everything + rowbuf[i]
    tot_out[...] = jnp.sqrt(everything[:, 0:4] / (scen * groups))


def write_out(min_, din, lin, norms, tot, mis_any, dual_any, lim_any, norm_any, tot_any, dual, lim, turned, sems):
    copies = [
        pltpu.make_async_copy(src, dst, sems.at[i])
        for i, (src, dst) in enumerate((
            (min_, mis_any), (tot, tot_any), (dual, dual_any), (lim, lim_any), (turned, norm_any),
        ))
    ]
    copies[0].start()
    copies[1].start()
    for k in range(din.shape[1]):
        dual[:, k * LANES : (k + 1) * LANES] = din[:, k, :]
    copies[2].start()
    for r in range(lin.shape[1]):
        lim[:, r * LANES : (r + 1) * LANES] = lin[:, r, :]
    copies[3].start()
    turned[...] = norms[...].T[0:4, :]
    copies[4].start()
    for copy in copies:
        copy.wait()


def per_device(
    base_vm, base_va, delta_state, multipliers, net_inj, ang_grad, from_bus, to_bus,
    status, conduct, suscept, charging, rating, slack, zdual,
):
    groups, ranks = lax.axis_size("ctg"), lax.axis_size("br")
    scen, _, nb = delta_state.shape
    nl = from_bus.shape[0]
    rows, btiles = nl // LANES, nb // LANES
    buses = nb * ranks
    tiles = buses // LANES
    high = -(-(buses // SPAN) // 16) * 16
    block = base_vm.shape[0]
    shares = 8
    share = -(-3 * rows // shares)
    f32, i32 = jnp.float32, jnp.int32
    vmem = pl.BlockSpec(memory_space=pltpu.VMEM)
    hbm = pl.BlockSpec(memory_space=pltpu.HBM)
    V = pltpu.VMEM
    outs = pl.pallas_call(
        functools.partial(body, groups, ranks),
        out_shape=(
            jax.ShapeDtypeStruct((ranks, 2, nb), f32),
            jax.ShapeDtypeStruct((ranks, btiles, LANES), f32),
            jax.ShapeDtypeStruct((ranks, rows, LANES), f32),
            jax.ShapeDtypeStruct((scen, LANES), f32),
            jax.ShapeDtypeStruct((1, 4), f32),
        ),
        in_specs=[hbm] * 15,
        out_specs=(vmem,) * 5,
        scratch_shapes=[
            V((1, block), f32), V((1, block), f32),
            V((scen, 2, nb), f32), V((scen, 2, nb), f32), V((scen, 2, nb), f32),
            V((scen, nb), f32), V((scen, nl), i32), V((scen, nl), f32), V((scen, nl), f32), V((rows, LANES), f32),
            V((scen, rows, LANES), i32), V((scen, rows, LANES), f32), V((scen, btiles, LANES), f32), V((scen, 1, LANES), f32),
            V((3, rows, LANES), f32), V((shares, share, LANES), f32), V((ranks, share, LANES), f32),
            V((shares, ranks, share, LANES), f32), V((ranks, 2, rows, LANES), i32),
            V((ranks, rows, LANES), i32),
            V((ranks, 2, nb), f32), V((ranks, 2, nb), f32), V((ranks, 2, LANES), f32), V((groups, 6, LANES), f32),
            V((ranks, 2, nb), f32), V((ranks, rows, LANES), f32), V((ranks, btiles, LANES), f32), V((ranks, 1, LANES), f32),
            V((4, tiles, LANES), f32), V((2 * tiles, 2 * LANES), jnp.bfloat16), V((2, ranks * rows, LANES), i32), V((3, ranks * rows, LANES), f32),
            V((ranks * rows, LANES), i32), V((4, ranks * rows, LANES), f32), V((ranks * rows, LANES), f32),
            V((2, SPAN // LANES, ranks * nl, LANES), jnp.bfloat16), V((6 * high, SPAN), f32),
            V((ranks, 2, nb), f32), V((ranks, btiles, LANES), f32), V((ranks, rows, LANES), f32),
            V((ranks, 1, LANES), f32), V((groups, 1, LANES), f32),
            pltpu.SemaphoreType.DMA((KINDS,)),
            pltpu.SemaphoreType.DMA((KINDS,)),
            pltpu.SemaphoreType.DMA((ranks,)),
            pltpu.SemaphoreType.DMA((ranks,)),
        ],
        compiler_params=pltpu.CompilerParams(
            collective_id=0, has_side_effects=True, vmem_limit_bytes=40 << 20
        ),
    )(*(pltpu.with_memory_space_constraint(x, pltpu.HBM) for x in (
        base_vm[None, :], base_va[None, :], delta_state, multipliers, net_inj, ang_grad,
        *(x.reshape(rows, LANES) for x in (from_bus, to_bus, conduct, suscept, charging, rating)),
        status, slack, zdual,
    )))
    mis, dual, lim, norms, tot = pl.pallas_call(
        write_out,
        out_shape=(
            jax.ShapeDtypeStruct((scen, 2, nb), f32),
            jax.ShapeDtypeStruct((scen, nb), f32),
            jax.ShapeDtypeStruct((scen, nl), f32),
            jax.ShapeDtypeStruct((4, scen), f32),
            jax.ShapeDtypeStruct((1, 4), f32),
        ),
        in_specs=[vmem] * 5,
        out_specs=(pl.BlockSpec(memory_space=pl.ANY),) * 5,
        scratch_shapes=[
            V((scen, nb), f32), V((scen, nl), f32), V((4, scen), f32), pltpu.SemaphoreType.DMA((5,)),
        ],
        compiler_params=pltpu.CompilerParams(vmem_limit_bytes=8 << 20),
    )(*outs)
    return (mis, dual, lim, norms.T, tot[0])


def solution(mesh):
    placed = (
        P(("ctg", "br")), P(("ctg", "br")),
        P("ctg", None, "br"), P("ctg", None, "br"), P("ctg", None, "br"), P("ctg", "br"),
        P("br"), P("br"), P("ctg", "br"), P("br"), P("br"), P("br"), P("br"),
        P("ctg", "br"), P("ctg", "br"),
    )
    return jax.shard_map(
        per_device,
        mesh=mesh,
        in_specs=placed,
        out_specs=(P("ctg", None, "br"), P("ctg", "br"), P("ctg", "br"), P("ctg", None), P()),
        check_vma=False,
    )
```
